32 devices in a mesh: dp: 32 (over z, y, x, core).
Axes of the slice: x: 2, y: 2, z: 4, core: 2. Of those that a mesh axis runs over, the one named last changes fastest.
Arguments:
- query_features: bfloat16 [8192, 768], P('dp'), may hold values from -24 to 24
- passage_features: bfloat16 [8192, 768], P('dp'), may hold values from -24 to 24
- counts: int32 [32], replicated, may hold values from 128 to 256, as said below
- positives: int32 [8192], P('dp'), may hold values from 0 to 4351
- w_first: bfloat16 [768, 1536], replicated, may hold values from -0.21875 to 0.21875
- w_second: bfloat16 [1536, 384], replicated, may hold values from -0.15625 to 0.15625
Outputs:
- mean_loss: float32 [], replicated
- grad_first: float32 [768, 1536], P(None, 'dp')
- grad_second: float32 [1536, 384], P('dp')
The draws below stay inside these ranges and needn't reach their ends.
Inputs may be any that keep to these rules, and one draw needn't show every extreme that they name: Device i holds counts[i] pairs in the first slots of its 256 slots. Each entry is 128 or 256; among the 16 devices whose indices agree modulo 32 // 16 exactly one entry is 256, so the entries sum to 4352. `positives`: only entries of occupied slots are used; an entry is the index of a passage in the order of occupied slots, device by device.
All inputs are finite; a program needn't handle non-finite values.
Results may differ from the reference program's by a relative error of at most 0.0043.
The reference program's roundings to bfloat16 on the way count: a program that leaves them out, or rounds other values in their place, can miss the bound.
Values may be sent and summed in bfloat16 or wider, within the bound.
A program may use at most 128 MiB of HBM per device.

```python
import jax
import jax.numpy as jnp
from jax import lax

D = 768
FF = 1536
E = 384
LOW = 128
BLOCK = 136
CAP = 256
PAIRS = 4352
N_DP = 32


def feature_pair(key):
    pass_key = jax.random.fold_in(key, 11)
    query_key = jax.random.fold_in(key, 12)
    shape = (N_DP * CAP, D)
    passages = jax.random.truncated_normal(pass_key, -4.0, 4.0, shape, jnp.float32)
    queries = jax.random.truncated_normal(query_key, -4.0, 4.0, shape, jnp.float32)
    return (queries, passages)


def draw_query_features(key, part):
    return feature_pair(key)[0].astype(jnp.bfloat16)


def draw_passage_features(key, part):
    return feature_pair(key)[1].astype(jnp.bfloat16)


def draw_counts(key, part):
    stride = N_DP // 16
    heavy_pos = jax.random.randint(key, (stride,), 0, 16)
    device_ids = jnp.arange(N_DP, dtype=jnp.int32)
    heavy = device_ids // stride == heavy_pos[device_ids % stride]
    return (LOW + LOW * heavy.astype(jnp.int32)).astype(jnp.int32)


def place_ends(values, rng, smallest, high):
    shape = values.shape
    index_at = [jax.random.randint(jax.random.fold_in(rng, axis), (), 0, shape[axis]) for axis in range(len(shape))]
    values = values.at[tuple(index_at)].set(smallest)
    longest = shape.index(max(shape))
    index_at[longest] = (index_at[longest] + 1) % shape[longest]
    return values.at[tuple(index_at)].set(high)


def normal_values(key, shape, spread, most, held_as=jnp.bfloat16):
    result = spread * jax.random.normal(key, shape, jnp.float32)
    return jnp.clip(result, min=-most, max=most).astype(held_as)


def setup_inputs(seed: int = 0) -> dict:
    keys = jax.random.split(jax.random.key(seed), 7)
    return {
        "query_features": draw_query_features(jax.random.fold_in(keys[6], 71), 0),
        "passage_features": draw_passage_features(jax.random.fold_in(keys[6], 71), 0),
        "counts": draw_counts(jax.random.fold_in(keys[6], 71), 0),
        "positives": place_ends(jax.random.randint(keys[3], (N_DP * CAP,), 0, PAIRS), jax.random.fold_in(keys[3], 1), 0, PAIRS - 1).astype(jnp.int32),
        "w_first": normal_values(keys[4], (D, FF), D ** -0.5, 0.21875),
        "w_second": normal_values(keys[5], (FF, E), FF ** -0.5, 0.15625),
    }


def gelu_tanh(values):
    return jax.nn.gelu(values, approximate=True)

def tower_pass(features, w_first, w_second):
    pre_act = jnp.dot(features, w_first, preferred_element_type=jnp.float32)
    hidden = gelu_tanh(pre_act).astype(jnp.bfloat16)
    embedded = jnp.dot(hidden, w_second, preferred_element_type=jnp.float32).astype(jnp.bfloat16)
    return (pre_act, hidden, embedded)

def weight_terms(features, pre_act, hidden, grads, w_second):
    grad_second = lax.dot_general(hidden, grads, (((0,), (0,)), ((), ())), preferred_element_type=jnp.float32)
    back_act = lax.dot_general(grads, w_second, (((1,), (1,)), ((), ())), preferred_element_type=jnp.float32)
    pull_back = jax.vjp(gelu_tanh, pre_act)[1]
    pre_grad = pull_back(back_act)[0].astype(jnp.bfloat16)
    grad_first = lax.dot_general(features, pre_grad, (((0,), (0,)), ((), ())), preferred_element_type=jnp.float32)
    return (grad_first, grad_second)

def reference(query_features, passage_features, counts, positives, w_first, w_second):
    slot_ids = jnp.arange(N_DP * CAP, dtype=jnp.int32)
    owner_dev = slot_ids // CAP
    row_in = slot_ids % CAP
    offsets = (jnp.cumsum(counts) - counts).astype(jnp.int32)
    occupied = row_in < counts[owner_dev]
    dest_row = jnp.where(occupied, offsets[owner_dev] + row_in, PAIRS).astype(jnp.int32)
    width = query_features.shape[1]
    queries_in = jnp.zeros((PAIRS, width), query_features.dtype).at[dest_row].set(query_features, mode='drop')
    passages_in = jnp.zeros((PAIRS, width), passage_features.dtype).at[dest_row].set(passage_features, mode='drop')
    positive_ids = jnp.zeros((PAIRS,), jnp.int32).at[dest_row].set(positives, mode='drop')
    pre_q, hidden_q, query_emb = tower_pass(queries_in, w_first, w_second)
    pre_p, hidden_p, passage_emb = tower_pass(passages_in, w_first, w_second)
    score_scale = 2.5 * E ** (-0.5)
    step_rows = BLOCK * 16
    step_count = PAIRS // step_rows
    columns = jnp.arange(PAIRS, dtype=jnp.int32)

    def one_step(grad_sum, step_index):
        query_rows = lax.dynamic_slice_in_dim(query_emb, step_index * step_rows, step_rows, 0)
        pos_rows = lax.dynamic_slice_in_dim(positive_ids, step_index * step_rows, step_rows, 0)
        scores = lax.dot_general(query_rows, passage_emb, (((1,), (1,)), ((), ())), preferred_element_type=jnp.float32) * score_scale
        row_top = lax.optimization_barrier(jnp.max(scores, axis=1))
        log_norm = row_top + jnp.log(lax.optimization_barrier(jnp.sum(jnp.exp(scores - row_top[:, None]), axis=1)))
        is_positive = pos_rows[:, None] == columns[None, :]
        pos_score = lax.optimization_barrier(jnp.sum(jnp.where(is_positive, scores, jnp.zeros_like(scores)), axis=1))
        weights = (jnp.exp(scores - log_norm[:, None]) - is_positive.astype(jnp.float32)).astype(jnp.bfloat16)
        query_grad = (score_scale * jnp.dot(weights, passage_emb, preferred_element_type=jnp.float32)).astype(jnp.bfloat16)
        grad_sum = grad_sum + lax.dot_general(weights, query_rows, (((0,), (0,)), ((), ())), preferred_element_type=jnp.float32)
        return (grad_sum, (query_grad, jnp.sum(log_norm - pos_score)))
    start_sum = jnp.zeros((PAIRS, query_emb.shape[1]), jnp.float32)
    grad_sum, (query_parts, loss_parts) = lax.scan(one_step, start_sum, jnp.arange(step_count, dtype=jnp.int32))
    query_grads = query_parts.reshape(PAIRS, query_emb.shape[1])
    passage_grads = (score_scale * grad_sum).astype(jnp.bfloat16)
    mean_loss = jnp.sum(loss_parts) / PAIRS
    first_q, second_q = weight_terms(queries_in, pre_q, hidden_q, query_grads, w_second)
    first_p, second_p = weight_terms(passages_in, pre_p, hidden_p, passage_grads, w_second)
    return (mean_loss, first_q + first_p, second_q + second_p)
```

```python
import functools

import jax
import jax.numpy as jnp
from jax import lax
from jax.experimental import pallas as pl
from jax.experimental.pallas import tpu as pltpu
from jax.sharding import PartitionSpec as P

MESH = pl.DeviceIdType.MESH
F32 = jnp.float32
BF16 = jnp.bfloat16


def gelu_tanh(values):
    return jax.nn.gelu(values, approximate=True)


def place_of(group, me, size, plane):
    count = size // plane
    if group == "plane":
        place = lax.rem(me, plane)
        return place, plane, 1, me - place
    if group == "line":
        return lax.div(me, plane), count, plane, lax.rem(me, plane)
    if group == "pair":
        place = lax.rem(me, 2)
        return place, 2, 1, me - place
    if group == "lane":
        place = lax.div(lax.rem(me, plane), 2)
        return place, plane // 2, 2, me - 2 * place
    stride = size // 16
    return lax.div(me, stride), 16, stride, lax.rem(me, stride)


def members_of(group, size, plane):
    return {"plane": plane, "line": size // plane, "pair": 2, "lane": plane // 2, "units": 16}[group]


def exchange_kernel(size, plane, plan, *refs):
    count = len(plan)
    sources, landings = refs[:count], refs[count : 2 * count]
    send_sem, recv_sem, own_sem = refs[2 * count :]
    me = lax.axis_index("dp")
    barrier = pltpu.get_barrier_semaphore()
    greeted = 0
    for group in sorted({group for group, _ in plan}):
        place, members, step, first = place_of(group, me, size, plane)
        for k in range(1, members):
            other = first + step * lax.rem(place + k, members)
            pl.semaphore_signal(barrier, inc=1, device_id=(other,), device_id_type=MESH)
            greeted += 1
    pl.semaphore_wait(barrier, greeted)
    copies = []
    used = 0
    for item, (group, kind) in enumerate(plan):
        place, members, step, first = place_of(group, me, size, plane)
        source, landing = sources[item], landings[item]
        for k in range(1, members):
            wrap = lax.div(place + k, members)
            there = place + k - members * wrap
            if kind == "gather":
                part = source
            elif kind == "scatter":
                part = source.at[there]
            elif kind == "column":
                part = source.at[:, there]
            else:
                part = source.at[there - 1 + wrap]
            copy = pltpu.make_async_remote_copy(
                src_ref=part,
                dst_ref=landing.at[place],
                send_sem=send_sem.at[used],
                recv_sem=recv_sem.at[used],
                device_id=(first + step * there,),
                device_id_type=MESH,
            )
            copy.start()
            copies.append(copy)
            used += 1
        if kind == "gather":
            own = pltpu.make_async_copy(source, landing.at[place], own_sem.at[item])
            own.start()
            copies.append(own)
    for copy in copies:
        copy.wait()


def exchange(name, size, plane, *items):
    plan = tuple((group, kind) for group, kind, _ in items)
    arrays = [array for _, _, array in items]
    shapes = []
    total = 0
    for group, kind, array in items:
        members = members_of(group, size, plane)
        total += members - 1
        if kind == "gather":
            block = array.shape
        elif kind == "column":
            block = array.shape[:1] + array.shape[2:]
        else:
            block = array.shape[1:]
        shapes.append(jax.ShapeDtypeStruct((members,) + block, array.dtype))
    return pl.pallas_call(
        functools.partial(exchange_kernel, size, plane, plan),
        out_shape=shapes,
        in_specs=[
            pl.BlockSpec(memory_space=pltpu.VMEM if kind == "gather" else pl.ANY) for _, kind in plan
        ],
        out_specs=[pl.BlockSpec(memory_space=pl.ANY)] * len(items),
        scratch_shapes=[
            pltpu.SemaphoreType.DMA((total,)),
            pltpu.SemaphoreType.DMA((total,)),
            pltpu.SemaphoreType.DMA((len(items),)),
        ],
        compiler_params=pltpu.CompilerParams(collective_id=name, has_side_effects=True),
    )(*arrays)


def last_kernel(size, plane, source, landing, send_sem, recv_sem):
    me = lax.axis_index("dp")
    rows = size // plane
    half = rows // 2
    row = lax.div(me, plane)
    core = lax.rem(me, 2)
    column = lax.rem(me, plane) - core
    barrier = pltpu.get_barrier_semaphore()
    spot = 2 * row + core
    for k in range(1, 2 * rows):
        other = lax.rem(spot + k, 2 * rows)
        index = plane * lax.div(other, 2) + column + lax.rem(other, 2)
        pl.semaphore_signal(barrier, inc=1, device_id=(index,), device_id_type=MESH)
    pl.semaphore_wait(barrier, 2 * rows - 1)
    sender_core = lax.div(row, half)

    def copy_of(i, j):
        return pltpu.make_async_remote_copy(
            src_ref=source.at[i, j],
            dst_ref=landing.at[row],
            send_sem=send_sem.at[i, j],
            recv_sem=recv_sem.at[row],
            device_id=(plane * (half * core + i) + column + j,),
            device_id_type=MESH,
        )

    for i in range(half):
        for j in range(2):
            target = plane * (half * core + i) + column + j

            @pl.when(target != me)
            def _():
                copy_of(i, j).start()

    for i in range(half):
        for j in range(2):
            target = plane * (half * core + i) + column + j

            @pl.when(target != me)
            def _():
                copy_of(i, j).wait_send()

    for sender_row in range(rows):
        sender = plane * sender_row + column + sender_core

        @pl.when(sender != me)
        def _():
            pltpu.make_async_remote_copy(
                src_ref=source.at[0, 0],
                dst_ref=landing.at[sender_row],
                send_sem=send_sem.at[0, 0],
                recv_sem=recv_sem.at[sender_row],
                device_id=(sender,),
                device_id_type=MESH,
            ).wait_recv()


def last_exchange(name, size, plane, chunks):
    rows = size // plane
    return pl.pallas_call(
        functools.partial(last_kernel, size, plane),
        out_shape=jax.ShapeDtypeStruct((rows,) + chunks.shape[2:], chunks.dtype),
        in_specs=[pl.BlockSpec(memory_space=pl.ANY)],
        out_specs=pl.BlockSpec(memory_space=pl.ANY),
        scratch_shapes=[
            pltpu.SemaphoreType.DMA((rows // 2, 2)),
            pltpu.SemaphoreType.DMA((rows,)),
        ],
        compiler_params=pltpu.CompilerParams(collective_id=name, has_side_effects=True),
    )(chunks)


def sum_with_own(own, arrived, place):
    slots = jnp.arange(arrived.shape[0], dtype=jnp.int32)
    mine = (slots == place).reshape((-1,) + (1,) * (arrived.ndim - 1))
    return jnp.sum(jnp.where(mine, own, arrived.astype(F32)), axis=0)


def body(query_features, passage_features, counts, positives, w_first, w_second):
    device_count = lax.axis_size("dp")
    plane = 1 << device_count.bit_length() // 2
    rows_of_planes = device_count // plane
    my_index = lax.axis_index("dp")
    stride = device_count // 16
    capacity, width = query_features.shape
    hidden_width, embed = w_second.shape
    base_rows = capacity // 2
    unit_rows = base_rows // 16
    block_rows = base_rows + unit_rows
    pair_count = block_rows * device_count
    score_scale = 2.5 * embed ** (-0.5)

    devices = jnp.arange(device_count, dtype=jnp.int32)
    group_of = devices % stride
    group_place = devices // stride
    heavy_dev = (counts > base_rows).astype(jnp.int32)
    same_mat = group_of[:, None] == group_of[None, :]
    heavy_place = jnp.sum(jnp.where(same_mat, (heavy_dev * group_place)[None, :], 0), axis=1)
    my_heavy = jnp.sum(jnp.where(devices == my_index, heavy_dev, 0))
    heavy_pos = jnp.sum(jnp.where(devices == my_index, heavy_place, 0))

    earlier_dev = devices[None, :] < devices[:, None]
    offsets = jnp.sum(jnp.where(earlier_dev, counts[None, :], 0), axis=1)
    inside = (offsets[None, :] <= positives[:, None]) & (
        positives[:, None] < (offsets + counts)[None, :]
    )
    owner_dev = jnp.sum(jnp.where(inside, devices[None, :], 0), axis=1)
    offset_row = positives - jnp.sum(jnp.where(inside, offsets[None, :], 0), axis=1)
    owner_heavy = jnp.sum(jnp.where(inside, heavy_place[None, :], 0), axis=1)
    beyond = jnp.maximum(offset_row - block_rows, 0)
    unit_ids = beyond // unit_rows
    target_place = unit_ids + (unit_ids >= owner_heavy).astype(jnp.int32)
    target = target_place * stride + owner_dev % stride
    new_pos = jnp.where(
        offset_row < block_rows,
        owner_dev * block_rows + offset_row,
        target * block_rows + base_rows + beyond % unit_rows,
    )
    lanes = jnp.arange(128, dtype=jnp.int32)
    coded = jnp.where(lanes[None, :] == 0, new_pos[:, None] // 256, new_pos[:, None] % 256)
    coded = jnp.where(lanes[None, :] < 2, coded, 0).astype(BF16)

    packed = jnp.concatenate([query_features, passage_features, coded], axis=1)
    units = packed[block_rows:].reshape(15, unit_rows, packed.shape[1])
    (arrived,) = exchange(0, device_count, plane, ("units", "unit", units))
    tail = lax.dynamic_index_in_dim(arrived, heavy_pos, 0, keepdims=False)
    tail = jnp.where(my_heavy == 1, packed[base_rows:block_rows], tail)
    tail_pos = (
        tail[:, 2 * width].astype(jnp.int32) * 256 + tail[:, 2 * width + 1].astype(jnp.int32)
    )
    own_pos = jnp.concatenate([new_pos[:base_rows], tail_pos])
    features = jnp.concatenate(
        [
            query_features[:base_rows],
            tail[:, :width],
            passage_features[:base_rows],
            tail[:, width : 2 * width],
        ],
        axis=0,
    )

    pre_act = jnp.dot(features, w_first, preferred_element_type=F32)
    hidden = gelu_tanh(pre_act).astype(BF16)
    embedded = jnp.dot(hidden, w_second, preferred_element_type=F32).astype(BF16)
    pos_tile = jnp.pad(own_pos, (0, 1024 - block_rows)).reshape(8, 128)
    queries, all_pos, passages, pair_features = exchange(
        1,
        device_count,
        plane,
        ("plane", "gather", embedded[:block_rows]),
        ("plane", "gather", pos_tile),
        ("line", "gather", embedded[block_rows:]),
        ("pair", "gather", features),
    )
    plane_place = my_index % plane
    line_place = my_index // plane
    queries = queries.reshape(plane * block_rows, embed)
    passages = passages.reshape(rows_of_planes * block_rows, embed)
    row_pos = all_pos.reshape(plane, 1024)[:, :block_rows].reshape(-1)
    columns = jnp.arange(rows_of_planes * block_rows, dtype=jnp.int32)
    columns = (
        columns // block_rows * plane + plane_place
    ) * block_rows + columns % block_rows

    scores = (
        lax.dot_general(queries, passages, (((1,), (1,)), ((), ())), preferred_element_type=F32)
        * score_scale
    )
    is_positive = row_pos[:, None] == columns[None, :]
    top = jnp.max(scores, axis=1)
    mass = jnp.sum(jnp.exp(scores - top[:, None]), axis=1)
    found = jnp.sum(jnp.where(is_positive, scores, 0.0), axis=1)
    stats = jnp.concatenate([part.reshape(plane, block_rows) for part in (top, mass, found)], axis=1)
    (all_stats,) = exchange(2, device_count, plane, ("plane", "gather", stats))
    tops, masses, founds = (
        all_stats[:, :, part * block_rows : (part + 1) * block_rows] for part in range(3)
    )
    row_top = jnp.max(tops, axis=0)
    log_norm = row_top + jnp.log(jnp.sum(masses * jnp.exp(tops - row_top[None]), axis=0))
    loss_part = jnp.sum(log_norm - jnp.sum(founds, axis=0))
    log_norm = log_norm.reshape(-1)
    weights = (jnp.exp(scores - log_norm[:, None]) - is_positive.astype(F32)).astype(BF16)
    query_part = score_scale * jnp.dot(weights, passages, preferred_element_type=F32)
    passage_part = score_scale * lax.dot_general(
        weights, queries, (((0,), (0,)), ((), ())), preferred_element_type=F32
    )
    query_part = query_part.reshape(plane, block_rows, embed)
    passage_part = passage_part.reshape(rows_of_planes, block_rows, embed)
    query_in, passage_in, losses = exchange(
        3,
        device_count,
        plane,
        ("plane", "scatter", query_part.astype(BF16)),
        ("line", "scatter", passage_part.astype(BF16)),
        ("line", "gather", jnp.broadcast_to(loss_part, (8, 128))),
    )
    mean_loss = jnp.sum(losses[:, 0, 0]) / pair_count
    grads = jnp.concatenate(
        [
            sum_with_own(query_part, query_in, plane_place),
            sum_with_own(passage_part, passage_in, line_place),
        ],
        axis=0,
    ).astype(BF16)
    (pair_grads,) = exchange(4, device_count, plane, ("pair", "gather", grads))

    core = my_index % 2
    half_width = hidden_width // 2
    first_half = lax.dynamic_slice_in_dim(w_first, core * half_width, half_width, 1)
    second_half = lax.dynamic_slice_in_dim(w_second, core * half_width, half_width, 0)
    both = pair_features.reshape(-1, width)
    both_grads = pair_grads.reshape(-1, embed)
    act = jnp.dot(both, first_half, preferred_element_type=F32)
    hid = gelu_tanh(act).astype(BF16)
    back = lax.dot_general(
        both_grads, second_half, (((1,), (1,)), ((), ())), preferred_element_type=F32
    )
    act_grad = jax.vjp(gelu_tanh, act)[1](back)[0].astype(BF16)
    grad_first = lax.dot_general(act_grad, both, (((0,), (0,)), ((), ())), preferred_element_type=F32)
    grad_second = lax.dot_general(hid, both_grads, (((0,), (0,)), ((), ())), preferred_element_type=F32)

    half = rows_of_planes // 2
    lanes_in_plane = plane // 2
    chunk = hidden_width // device_count
    own_first = grad_first.reshape(half, lanes_in_plane, 2 * chunk, width)
    own_second = grad_second.reshape(half, lanes_in_plane, 2 * chunk, embed)
    first_in, second_in = exchange(
        5,
        device_count,
        plane,
        ("lane", "column", own_first.astype(BF16)),
        ("lane", "column", own_second.astype(BF16)),
    )
    lane_place = plane_place // 2
    sum_first = sum_with_own(
        jnp.swapaxes(own_first, 0, 1), first_in, lane_place
    ).reshape(half, 2, chunk, width)
    sum_second = sum_with_own(
        jnp.swapaxes(own_second, 0, 1), second_in, lane_place
    ).reshape(half, 2, chunk, embed)
    chunks = jnp.concatenate([sum_first, sum_second], axis=3)
    landed = last_exchange(6, device_count, plane, chunks.astype(BF16))
    own_chunk = chunks[line_place % half, core]
    slots = jnp.arange(rows_of_planes, dtype=jnp.int32)
    mine = (slots == line_place) & (line_place // half == core)
    total = jnp.sum(jnp.where(mine[:, None, None], own_chunk[None], landed.astype(F32)), axis=0)
    return (mean_loss, total[:, :width].T, total[:, width:])


def solution(mesh):
    return jax.shard_map(
        body,
        mesh=mesh,
        in_specs=(P("dp", None), P("dp", None), P(), P("dp"), P(), P()),
        out_specs=(P(), P(None, "dp"), P("dp", None)),
        check_vma=False,
    )
```

```python
import functools

import jax
import jax.numpy as jnp
from jax import lax
from jax.experimental import pallas as pl
from jax.experimental.pallas import tpu as pltpu
from jax.sharding import PartitionSpec as P

MESH = pl.DeviceIdType.MESH
F32 = jnp.float32
BF16 = jnp.bfloat16


def gelu_tanh(values):
    return jax.nn.gelu(values, approximate=True)


def place_of(group, me, size, plane):
    count = size // plane
    if group == "plane":
        place = lax.rem(me, plane)
        return place, plane, 1, me - place
    if group == "line":
        return lax.div(me, plane), count, plane, lax.rem(me, plane)
    if group == "pair":
        place = lax.rem(me, 2)
        return place, 2, 1, me - place
    if group == "lane":
        place = lax.div(lax.rem(me, plane), 2)
        return place, plane // 2, 2, me - 2 * place
    stride = size // 16
    return lax.div(me, stride), 16, stride, lax.rem(me, stride)


def members_of(group, size, plane):
    return {"plane": plane, "line": size // plane, "pair": 2, "lane": plane // 2, "units": 16}[group]


def exchange_kernel(size, plane, plan, *refs):
    count = len(plan)
    sources, landings = refs[:count], refs[count : 2 * count]
    send_sem, recv_sem, own_sem = refs[2 * count :]
    me = lax.axis_index("dp")
    barrier = pltpu.get_barrier_semaphore()
    greeted = 0
    for group in sorted({group for group, _ in plan}):
        place, members, step, first = place_of(group, me, size, plane)
        for k in range(1, members):
            other = first + step * lax.rem(place + k, members)
            pl.semaphore_signal(barrier, inc=1, device_id=(other,), device_id_type=MESH)
            greeted += 1
    pl.semaphore_wait(barrier, greeted)
    copies = []
    used = 0
    for item, (group, kind) in enumerate(plan):
        place, members, step, first = place_of(group, me, size, plane)
        source, landing = sources[item], landings[item]
        for k in range(1, members):
            wrap = lax.div(place + k, members)
            there = place + k - members * wrap
            if kind == "gather":
                part = source
            elif kind == "scatter":
                part = source.at[there]
            elif kind == "column":
                part = source.at[:, there]
            else:
                part = source.at[there - 1 + wrap]
            copy = pltpu.make_async_remote_copy(
                src_ref=part,
                dst_ref=landing.at[place],
                send_sem=send_sem.at[used],
                recv_sem=recv_sem.at[used],
                device_id=(first + step * there,),
                device_id_type=MESH,
            )
            copy.start()
            copies.append(copy)
            used += 1
        if kind == "gather":
            own = pltpu.make_async_copy(source, landing.at[place], own_sem.at[item])
            own.start()
            copies.append(own)
    for copy in copies:
        copy.wait()


def exchange(name, size, plane, *items):
    plan = tuple((group, kind) for group, kind, _ in items)
    arrays = [array for _, _, array in items]
    shapes = []
    total = 0
    for group, kind, array in items:
        members = members_of(group, size, plane)
        total += members - 1
        if kind == "gather":
            block = array.shape
        elif kind == "column":
            block = array.shape[:1] + array.shape[2:]
        else:
            block = array.shape[1:]
        shapes.append(jax.ShapeDtypeStruct((members,) + block, array.dtype))
    return pl.pallas_call(
        functools.partial(exchange_kernel, size, plane, plan),
        out_shape=shapes,
        in_specs=[
            pl.BlockSpec(memory_space=pltpu.VMEM if kind == "gather" else pl.ANY) for _, kind in plan
        ],
        out_specs=[pl.BlockSpec(memory_space=pl.ANY)] * len(items),
        scratch_shapes=[
            pltpu.SemaphoreType.DMA((total,)),
            pltpu.SemaphoreType.DMA((total,)),
            pltpu.SemaphoreType.DMA((len(items),)),
        ],
        compiler_params=pltpu.CompilerParams(collective_id=name, has_side_effects=True),
    )(*arrays)


GELU_ROOT = 0.7978845608028654
GELU_CUBE = 0.044715


def gelu_and_slope(value):
    square = value * value
    bent = jnp.tanh(GELU_ROOT * value * (1.0 + GELU_CUBE * square))
    rise = 0.5 * (1.0 + bent)
    slope = rise + 0.5 * value * (1.0 - bent * bent) * (
        GELU_ROOT * (1.0 + 3.0 * GELU_CUBE * square)
    )
    return value * rise, slope


def dot(left, right, left_dim, right_dim):
    return lax.dot_general(
        left, right, (((left_dim,), (right_dim,)), ((), ())), preferred_element_type=F32
    )


TILES = 2


def tail_kernel(
    size,
    plane,
    features,
    grads,
    w_first,
    w_second,
    out_first,
    out_second,
    both_grads,
    own,
    outgoing,
    landing,
    sums,
    forward,
    landed,
    pair_sems,
    lane_send,
    lane_recv,
    line_send,
    line_recv,
):
    me = lax.axis_index("dp")
    rows = size // plane
    half = rows // 2
    lanes = plane // 2
    row = lax.div(me, plane)
    core = lax.rem(me, 2)
    lane = lax.div(lax.rem(me, plane), 2)
    column = lax.rem(me, plane) - core
    width = features.shape[1]
    local_rows = grads.shape[0]
    hidden_half = w_second.shape[0] // 2
    tile = hidden_half // TILES
    per_tile = half // TILES
    chunk = hidden_half // (half * lanes * 2)

    barrier = pltpu.get_barrier_semaphore()
    spot = 2 * row + core
    for k in range(1, 2 * rows):
        other = lax.rem(spot + k, 2 * rows)
        index = plane * lax.div(other, 2) + column + lax.rem(other, 2)
        pl.semaphore_signal(barrier, inc=1, device_id=(index,), device_id_type=MESH)
    for k in range(1, lanes):
        index = plane * row + 2 * lax.rem(lane + k, lanes) + core
        pl.semaphore_signal(barrier, inc=1, device_id=(index,), device_id_type=MESH)
    pl.semaphore_wait(barrier, 2 * rows + lanes - 2)

    pair_copy = pltpu.make_async_remote_copy(
        src_ref=grads,
        dst_ref=both_grads.at[core],
        send_sem=pair_sems.at[0],
        recv_sem=pair_sems.at[1],
        device_id=(me + 1 - 2 * core,),
        device_id_type=MESH,
    )
    pair_copy.start()
    both_grads[core] = grads[...]

    def lane_copy(t, k):
        there = lax.rem(lane + k, lanes)
        return pltpu.make_async_remote_copy(
            src_ref=outgoing.at[pl.ds(t * per_tile, per_tile), there],
            dst_ref=landing.at[lane, pl.ds(t * per_tile, per_tile)],
            send_sem=lane_send.at[t, k],
            recv_sem=lane_recv.at[t, k],
            device_id=(plane * row + 2 * there + core,),
            device_id_type=MESH,
        )

    for t in range(TILES):
        start = pl.multiple_of(core * hidden_half + t * tile, 128)
        act = dot(features[...], w_first[:, pl.ds(start, tile)], 1, 0)
        hidden, slope = gelu_and_slope(act)
        hidden = hidden.astype(BF16)
        if t == 0:
            pair_copy.wait()
        de = both_grads[...].reshape(2 * local_rows, -1)
        back = dot(de, w_second[pl.ds(start, tile), :], 1, 1)
        act_grad = (slope * back).astype(BF16)
        first = dot(act_grad, features[...], 0, 0)
        second = dot(hidden, de, 0, 0)
        for i in range(per_tile):
            for m in range(lanes):
                for j in range(2):
                    at = ((i * lanes + m) * 2 + j) * chunk
                    for part, low in ((first, 0), (second, width)):
                        high = low + part.shape[1]
                        piece = part[at : at + chunk]
                        own[t * per_tile + i, m, j, :, low:high] = piece
                        outgoing[t * per_tile + i, m, j, :, low:high] = piece.astype(BF16)
        for k in range(1, lanes):
            lane_copy(t, k).start()

    sender_core = lax.div(row, half)

    def line_copy(i, j):
        return pltpu.make_async_remote_copy(
            src_ref=forward.at[i, j],
            dst_ref=landed.at[row],
            send_sem=line_send.at[i, j],
            recv_sem=line_recv.at[row],
            device_id=(plane * (half * core + i) + column + j,),
            device_id_type=MESH,
        )

    for t in range(TILES):
        for k in range(1, lanes):
            lane_copy(t, k).wait()
        for i in range(t * per_tile, (t + 1) * per_tile):
            for j in range(2):
                total = own[i, lane, j]
                for k in range(1, lanes):
                    total = total + landing[lax.rem(lane + k, lanes), i, j].astype(F32)
                sums[i, j] = total
                forward[i, j] = total.astype(BF16)

                @pl.when(plane * (half * core + i) + column + j != me)
                def _():
                    line_copy(i, j).start()

    for i in range(half):
        for j in range(2):

            @pl.when(plane * (half * core + i) + column + j != me)
            def _():
                line_copy(i, j).wait_send()

    for sender_row in range(rows):
        sender = plane * sender_row + column + sender_core

        @pl.when(sender != me)
        def _():
            pltpu.make_async_remote_copy(
                src_ref=forward.at[0, 0],
                dst_ref=landed.at[sender_row],
                send_sem=line_send.at[0, 0],
                recv_sem=line_recv.at[sender_row],
                device_id=(sender,),
                device_id_type=MESH,
            ).wait_recv()

    total = jnp.where(sender_core == core, sums[lax.rem(row, half), core], 0.0)
    for sender_row in range(rows):
        sender = plane * sender_row + column + sender_core
        total = total + jnp.where(sender == me, 0.0, landed[sender_row].astype(F32))
    out_first[...] = total[:, :width]
    out_second[...] = total[:, width:]


def finish(name, size, plane, features, grads, w_first, w_second):
    rows, lanes = size // plane, plane // 2
    half = rows // 2
    width, hidden_width = w_first.shape
    embed = w_second.shape[1]
    chunk = hidden_width // size
    across = width + embed
    vmem = pl.BlockSpec(memory_space=pltpu.VMEM)
    return pl.pallas_call(
        functools.partial(tail_kernel, size, plane),
        out_shape=[
            jax.ShapeDtypeStruct((chunk, width), F32),
            jax.ShapeDtypeStruct((chunk, embed), F32),
        ],
        in_specs=[vmem] * 4,
        out_specs=[vmem] * 2,
        scratch_shapes=[
            pltpu.VMEM((2,) + grads.shape, BF16),
            pltpu.VMEM((half, lanes, 2, chunk, across), F32),
            pltpu.VMEM((half, lanes, 2, chunk, across), BF16),
            pltpu.VMEM((lanes, half, 2, chunk, across), BF16),
            pltpu.VMEM((half, 2, chunk, across), F32),
            pltpu.VMEM((half, 2, chunk, across), BF16),
            pltpu.VMEM((rows, chunk, across), BF16),
            pltpu.SemaphoreType.DMA((2,)),
            pltpu.SemaphoreType.DMA((TILES, lanes)),
            pltpu.SemaphoreType.DMA((TILES, lanes)),
            pltpu.SemaphoreType.DMA((half, 2)),
            pltpu.SemaphoreType.DMA((rows,)),
        ],
        compiler_params=pltpu.CompilerParams(
            collective_id=name, has_side_effects=True, vmem_limit_bytes=50 * 1024 * 1024
        ),
    )(features, grads, w_first, w_second)


def sum_with_own(own, arrived, place):
    slots = jnp.arange(arrived.shape[0], dtype=jnp.int32)
    mine = (slots == place).reshape((-1,) + (1,) * (arrived.ndim - 1))
    return jnp.sum(jnp.where(mine, own, arrived.astype(F32)), axis=0)


def body(query_features, passage_features, counts, positives, w_first, w_second):
    device_count = lax.axis_size("dp")
    plane = 1 << device_count.bit_length() // 2
    rows_of_planes = device_count // plane
    my_index = lax.axis_index("dp")
    stride = device_count // 16
    capacity, width = query_features.shape
    hidden_width, embed = w_second.shape
    base_rows = capacity // 2
    unit_rows = base_rows // 16
    block_rows = base_rows + unit_rows
    pair_count = block_rows * device_count
    score_scale = 2.5 * embed ** (-0.5)

    devices = jnp.arange(device_count, dtype=jnp.int32)
    group_of = devices % stride
    group_place = devices // stride
    heavy_dev = (counts > base_rows).astype(jnp.int32)
    same_mat = group_of[:, None] == group_of[None, :]
    heavy_place = jnp.sum(jnp.where(same_mat, (heavy_dev * group_place)[None, :], 0), axis=1)
    my_heavy = jnp.sum(jnp.where(devices == my_index, heavy_dev, 0))
    heavy_pos = jnp.sum(jnp.where(devices == my_index, heavy_place, 0))

    earlier_dev = devices[None, :] < devices[:, None]
    offsets = jnp.sum(jnp.where(earlier_dev, counts[None, :], 0), axis=1)
    inside = (offsets[None, :] <= positives[:, None]) & (
        positives[:, None] < (offsets + counts)[None, :]
    )
    owner_dev = jnp.sum(jnp.where(inside, devices[None, :], 0), axis=1)
    offset_row = positives - jnp.sum(jnp.where(inside, offsets[None, :], 0), axis=1)
    owner_heavy = jnp.sum(jnp.where(inside, heavy_place[None, :], 0), axis=1)
    beyond = jnp.maximum(offset_row - block_rows, 0)
    unit_ids = beyond // unit_rows
    target_place = unit_ids + (unit_ids >= owner_heavy).astype(jnp.int32)
    target = target_place * stride + owner_dev % stride
    new_pos = jnp.where(
        offset_row < block_rows,
        owner_dev * block_rows + offset_row,
        target * block_rows + base_rows + beyond % unit_rows,
    )
    lanes = jnp.arange(128, dtype=jnp.int32)
    coded = jnp.where(lanes[None, :] == 0, new_pos[:, None] // 256, new_pos[:, None] % 256)
    coded = jnp.where(lanes[None, :] < 2, coded, 0).astype(BF16)

    packed = jnp.concatenate([query_features, passage_features, coded], axis=1)
    units = packed[block_rows:].reshape(15, unit_rows, packed.shape[1])
    (arrived,) = exchange(0, device_count, plane, ("units", "unit", units))
    tail = lax.dynamic_index_in_dim(arrived, heavy_pos, 0, keepdims=False)
    tail = jnp.where(my_heavy == 1, packed[base_rows:block_rows], tail)
    tail_pos = (
        tail[:, 2 * width].astype(jnp.int32) * 256 + tail[:, 2 * width + 1].astype(jnp.int32)
    )
    own_pos = jnp.concatenate([new_pos[:base_rows], tail_pos])
    features = jnp.concatenate(
        [
            query_features[:base_rows],
            tail[:, :width],
            passage_features[:base_rows],
            tail[:, width : 2 * width],
        ],
        axis=0,
    )

    pre_act = jnp.dot(features, w_first, preferred_element_type=F32)
    hidden = gelu_tanh(pre_act).astype(BF16)
    embedded = jnp.dot(hidden, w_second, preferred_element_type=F32).astype(BF16)
    pos_tile = jnp.pad(own_pos, (0, 1024 - block_rows)).reshape(8, 128)
    queries, all_pos, passages, pair_features = exchange(
        1,
        device_count,
        plane,
        ("plane", "gather", embedded[:block_rows]),
        ("plane", "gather", pos_tile),
        ("line", "gather", embedded[block_rows:]),
        ("pair", "gather", features),
    )
    plane_place = my_index % plane
    line_place = my_index // plane
    queries = queries.reshape(plane * block_rows, embed)
    passages = passages.reshape(rows_of_planes * block_rows, embed)
    row_pos = all_pos.reshape(plane, 1024)[:, :block_rows].reshape(-1)
    columns = jnp.arange(rows_of_planes * block_rows, dtype=jnp.int32)
    columns = (
        columns // block_rows * plane + plane_place
    ) * block_rows + columns % block_rows

    scores = (
        lax.dot_general(queries, passages, (((1,), (1,)), ((), ())), preferred_element_type=F32)
        * score_scale
    )
    is_positive = row_pos[:, None] == columns[None, :]
    top = jnp.max(scores, axis=1)
    mass = jnp.sum(jnp.exp(scores - top[:, None]), axis=1)
    found = jnp.sum(jnp.where(is_positive, scores, 0.0), axis=1)
    stats = jnp.concatenate([part.reshape(plane, block_rows) for part in (top, mass, found)], axis=1)
    (all_stats,) = exchange(2, device_count, plane, ("plane", "gather", stats))
    tops, masses, founds = (
        all_stats[:, :, part * block_rows : (part + 1) * block_rows] for part in range(3)
    )
    row_top = jnp.max(tops, axis=0)
    log_norm = row_top + jnp.log(jnp.sum(masses * jnp.exp(tops - row_top[None]), axis=0))
    loss_part = jnp.sum(log_norm - jnp.sum(founds, axis=0))
    log_norm = log_norm.reshape(-1)
    weights = (jnp.exp(scores - log_norm[:, None]) - is_positive.astype(F32)).astype(BF16)
    query_part = score_scale * jnp.dot(weights, passages, preferred_element_type=F32)
    passage_part = score_scale * lax.dot_general(
        weights, queries, (((0,), (0,)), ((), ())), preferred_element_type=F32
    )
    query_part = query_part.reshape(plane, block_rows, embed)
    passage_part = passage_part.reshape(rows_of_planes, block_rows, embed)
    query_in, passage_in, losses = exchange(
        3,
        device_count,
        plane,
        ("plane", "scatter", query_part.astype(BF16)),
        ("line", "scatter", passage_part.astype(BF16)),
        ("line", "gather", jnp.broadcast_to(loss_part, (8, 128))),
    )
    mean_loss = jnp.sum(losses[:, 0, 0]) / pair_count
    grads = jnp.concatenate(
        [
            sum_with_own(query_part, query_in, plane_place),
            sum_with_own(passage_part, passage_in, line_place),
        ],
        axis=0,
    ).astype(BF16)
    total_first, total_second = finish(
        4, device_count, plane, pair_features.reshape(-1, width), grads, w_first, w_second
    )
    return (mean_loss, total_first.T, total_second)


def solution(mesh):
    return jax.shard_map(
        body,
        mesh=mesh,
        in_specs=(P("dp", None), P("dp", None), P(), P("dp"), P(), P()),
        out_specs=(P(), P(None, "dp"), P("dp", None)),
        check_vma=False,
    )
```

```python
import functools

import jax
import jax.numpy as jnp
from jax import lax
from jax.experimental import pallas as pl
from jax.experimental.pallas import tpu as pltpu
from jax.sharding import PartitionSpec as P

MESH = pl.DeviceIdType.MESH
F32 = jnp.float32
BF16 = jnp.bfloat16
GELU_ROOT = 0.7978845608028654
GELU_CUBE = 0.044715
TILES = 2


def gelu_and_slope(value):
    square = value * value
    bent = jnp.tanh(GELU_ROOT * value * (1.0 + GELU_CUBE * square))
    rise = 0.5 * (1.0 + bent)
    slope = rise + 0.5 * value * (1.0 - bent * bent) * (
        GELU_ROOT * (1.0 + 3.0 * GELU_CUBE * square)
    )
    return value * rise, slope


def dot(left, right, left_dim, right_dim):
    return lax.dot_general(
        left, right, (((left_dim,), (right_dim,)), ((), ())), preferred_element_type=F32
    )


def flat_rows(blocks):
    return blocks.astype(F32).reshape(-1, blocks.shape[-1]).astype(BF16)


class Copies:
    def __init__(self, send, recv):
        self.send, self.recv, self.used = send, recv, 0

    def start(self, source, landing, device):
        copy = pltpu.make_async_remote_copy(
            src_ref=source,
            dst_ref=landing,
            send_sem=self.send.at[self.used],
            recv_sem=self.recv.at[self.used],
            device_id=(device,),
            device_id_type=MESH,
        )
        self.used += 1
        copy.start()
        return copy


def wait_all(copies):
    for copy in copies:
        copy.wait()


def step_kernel(
    size,
    plane,
    score_scale,
    facts,
    query_features,
    passage_features,
    own_code,
    base_pos,
    units,
    w_first,
    w_second,
    out_loss,
    out_first,
    out_second,
    unit_land,
    feat_base,
    feat_tail,
    q_base,
    q_tail,
    p_base,
    p_tail,
    pos_land,
    all_q,
    all_p,
    scores,
    stat_land,
    dq_own_base,
    dq_own_tail,
    dq_out_base,
    dq_out_tail,
    dq_land_base,
    dq_land_tail,
    dp_own_base,
    dp_own_tail,
    dp_out_base,
    dp_out_tail,
    dp_land_base,
    dp_land_tail,
    loss_land,
    de_base,
    de_tail,
    all_x,
    own,
    outgoing,
    landing,
    sums,
    forward,
    landed,
    send_sems,
    recv_sems,
    line_send,
    line_recv,
):
    me = lax.axis_index("dp")
    rows = size // plane
    half = rows // 2
    lanes = plane // 2
    stride = size // 16
    row = lax.div(me, plane)
    spot = lax.rem(me, plane)
    core = lax.rem(me, 2)
    lane = lax.div(spot, 2)
    column = spot - core
    place = lax.div(me, stride)
    partner = me + 1 - 2 * core
    width, hidden_width = w_first.shape
    embed = w_second.shape[1]
    base = q_base.shape[1]
    unit = q_tail.shape[1]
    hidden_half = hidden_width // 2
    tile = hidden_half // TILES
    per_tile = half // TILES
    chunk = hidden_half // (half * lanes * 2)
    copies = Copies(send_sems, recv_sems)

    plane_peers = [row * plane + lax.rem(spot + k, plane) for k in range(1, plane)]
    line_peers = [lax.rem(row + k, rows) * plane + spot for k in range(1, rows)]
    barrier = pltpu.get_barrier_semaphore()

    def greet(device):
        pl.semaphore_signal(barrier, inc=1, device_id=(device,), device_id_type=MESH)

    for k in range(1, 16):
        greet(lax.rem(place + k, 16) * stride + lax.rem(me, stride))
    for device in plane_peers:
        greet(device)
    in_column = 2 * row + core
    for k in range(1, 2 * rows):
        other = lax.rem(in_column + k, 2 * rows)
        greet(plane * lax.div(other, 2) + column + lax.rem(other, 2))
    pl.semaphore_wait(barrier, 15 + plane - 1 + 2 * rows - 1)

    unit_copies = []
    for k in range(1, 16):
        wrap = lax.div(place + k, 16)
        there = place + k - 16 * wrap
        unit_copies.append(
            copies.start(
                units.at[there - 1 + wrap],
                unit_land.at[place],
                there * stride + lax.rem(me, stride),
            )
        )

    def tower(features):
        total = None
        for low in range(0, hidden_width, tile):
            act = dot(features, w_first[:, low : low + tile], 1, 0)
            hidden = gelu_and_slope(act)[0].astype(BF16)
            part = dot(hidden, w_second[low : low + tile, :], 1, 0)
            total = part if total is None else total + part
        return total.astype(BF16)

    feat_base[core, 0] = query_features[:base]
    feat_base[core, 1] = passage_features[:base]
    pair_x = [copies.start(feat_base.at[core], feat_base.at[core], partner)]
    embedded = tower(feat_base[core].reshape(2 * base, width))
    q_base[spot] = embedded[:base]
    p_base[row] = embedded[base:]
    q_copies = [copies.start(q_base.at[spot], q_base.at[spot], device) for device in plane_peers]
    p_copies = [copies.start(p_base.at[row], p_base.at[row], device) for device in line_peers]

    wait_all(unit_copies)
    heavy = facts[0, 1] == 1
    got = unit_land[facts[0, 0]].astype(F32)
    tail_q = jnp.where(heavy, query_features[base : base + unit].astype(F32), got[:, :width])
    tail_p = jnp.where(
        heavy, passage_features[base : base + unit].astype(F32), got[:, width : 2 * width]
    )
    code = jnp.where(heavy, own_code[...].astype(F32), got[:, 2 * width :])
    tail_pos = code[:, :1] * 256.0 + code[:, 1:2]
    tail_x = jnp.concatenate([tail_q, tail_p], axis=0)
    feat_tail[core] = tail_x.reshape(2, unit, width).astype(BF16)
    tail_e = tower(tail_x.astype(BF16)).astype(F32)
    q_tail[spot] = tail_e[:unit].astype(BF16)
    p_tail[row] = tail_e[unit:].astype(BF16)
    pos_land[spot, 0] = base_pos[...]
    sub = lax.broadcasted_iota(jnp.int32, (unit, base), 0) + spot * unit
    along = lax.broadcasted_iota(jnp.int32, (unit, base), 1)
    pos_land[spot, 1] = jnp.sum(jnp.where(sub == along, tail_pos, 0.0), axis=0, keepdims=True)
    for device in plane_peers:
        q_copies.append(copies.start(pos_land.at[spot], pos_land.at[spot], device))
        q_copies.append(copies.start(q_tail.at[spot], q_tail.at[spot], device))
    for device in line_peers:
        p_copies.append(copies.start(p_tail.at[row], p_tail.at[row], device))
    pair_x.append(copies.start(feat_tail.at[core], feat_tail.at[core], partner))
    wait_all(q_copies)
    wait_all(p_copies)

    q_rows, p_rows = plane * base, rows * base
    all_q[:q_rows] = q_base[...].reshape(q_rows, embed)
    all_q[q_rows:] = flat_rows(q_tail[...])
    all_p[:p_rows] = p_base[...].reshape(p_rows, embed)
    all_p[p_rows:] = flat_rows(p_tail[...])
    pos_tail = pos_land[0, 1]
    for k in range(1, plane):
        pos_tail = pos_tail + pos_land[k, 1]
    wanted = jnp.concatenate(
        [pos_land[k, 0] for k in range(plane)] + [pos_tail[:, : plane * unit]], axis=1
    )
    ids = jnp.concatenate(
        [lax.broadcasted_iota(jnp.int32, (base, 1), 0) + facts[1, k] for k in range(rows)]
        + [lax.broadcasted_iota(jnp.int32, (unit, 1), 0) + facts[2, k] for k in range(rows)],
        axis=0,
    ).astype(F32)
    scores[...] = score_scale * dot(all_p[...], all_q[...], 1, 1)
    value = scores[...]
    hit = ids == wanted
    top = jnp.max(value, axis=0, keepdims=True)
    stat_land[spot, 0:1] = top
    stat_land[spot, 1:2] = jnp.sum(jnp.exp(value - top), axis=0, keepdims=True)
    stat_land[spot, 2:3] = jnp.sum(jnp.where(hit, value, 0.0), axis=0, keepdims=True)
    stat_land[spot, 3:4] = jnp.zeros_like(top)
    wait_all(
        [copies.start(stat_land.at[spot], stat_land.at[spot], device) for device in plane_peers]
    )
    stats = stat_land[...]
    tops = stats[:, 0]
    row_top = jnp.max(tops, axis=0, keepdims=True)
    mass = jnp.sum(stats[:, 1] * jnp.exp(tops - row_top), axis=0, keepdims=True)
    log_norm = row_top + jnp.log(mass)
    found = jnp.sum(stats[:, 2], axis=0, keepdims=True)
    loss_land[row] = jnp.broadcast_to(
        jnp.sum(log_norm - found, axis=1, keepdims=True), loss_land.shape[1:]
    )
    grads_t = (jnp.exp(scores[...] - log_norm) - hit.astype(F32)).astype(BF16)

    def scatter(part, own_base, own_tail, out_base, out_tail, land_base, land_tail, mine, peers):
        split = own_base.shape[0] * base
        own_base[...] = part[:split].reshape(own_base.shape)
        own_tail[...] = part[split:].reshape(own_tail.shape)
        out_base[...] = own_base[...].astype(out_base.dtype)
        out_tail[...] = own_tail[...].astype(out_tail.dtype)
        made = []
        for there, device in peers:
            made.append(copies.start(out_base.at[there], land_base.at[mine], device))
            made.append(copies.start(out_tail.at[there], land_tail.at[mine], device))
        return made

    def gathered(own_part, land, mine, members):
        total = own_part[mine]
        for k in range(1, members):
            total = total + land[lax.rem(mine + k, members)].astype(F32)
        return total.astype(BF16)

    dq_copies = scatter(
        score_scale * dot(grads_t, all_p[...], 0, 0),
        dq_own_base,
        dq_own_tail,
        dq_out_base,
        dq_out_tail,
        dq_land_base,
        dq_land_tail,
        spot,
        [(lax.rem(spot + k, plane), plane_peers[k - 1]) for k in range(1, plane)],
    )
    dp_copies = scatter(
        score_scale * dot(grads_t, all_q[...], 1, 0),
        dp_own_base,
        dp_own_tail,
        dp_out_base,
        dp_out_tail,
        dp_land_base,
        dp_land_tail,
        row,
        [(lax.rem(row + k, rows), line_peers[k - 1]) for k in range(1, rows)],
    )
    loss_copies = [
        copies.start(loss_land.at[row], loss_land.at[row], device) for device in line_peers
    ]
    wait_all(pair_x)
    x_rows = 4 * base
    all_x[:x_rows] = feat_base[...].reshape(x_rows, width)
    all_x[x_rows:] = flat_rows(feat_tail[...])
    wait_all(dq_copies)
    de_base[core, 0] = gathered(dq_own_base, dq_land_base, spot, plane)
    de_tail[core, 0] = gathered(dq_own_tail, dq_land_tail, spot, plane)
    wait_all(dp_copies)
    de_base[core, 1] = gathered(dp_own_base, dp_land_base, row, rows)
    de_tail[core, 1] = gathered(dp_own_tail, dp_land_tail, row, rows)
    pair_de = [
        copies.start(de_base.at[core], de_base.at[core], partner),
        copies.start(de_tail.at[core], de_tail.at[core], partner),
    ]
    wait_all(loss_copies)
    loss = loss_land[0]
    for k in range(1, rows):
        loss = loss + loss_land[k]
    out_loss[...] = loss

    lane_copies = []
    for t in range(TILES):
        start = pl.multiple_of(core * hidden_half + t * tile, 128)
        act = dot(all_x[...], w_first[:, pl.ds(start, tile)], 1, 0)
        hidden, slope = gelu_and_slope(act)
        hidden = hidden.astype(BF16)
        if t == 0:
            wait_all(pair_de)
        de = jnp.concatenate(
            [de_base[...].reshape(x_rows, embed), flat_rows(de_tail[...])], axis=0
        )
        back = dot(de, w_second[pl.ds(start, tile), :], 1, 1)
        act_grad = (slope * back).astype(BF16)
        first = dot(act_grad, all_x[...], 0, 0)
        second = dot(hidden, de, 0, 0)
        for i in range(per_tile):
            for m in range(lanes):
                for j in range(2):
                    at = ((i * lanes + m) * 2 + j) * chunk
                    for part, low in ((first, 0), (second, width)):
                        high = low + part.shape[1]
                        piece = part[at : at + chunk]
                        own[t * per_tile + i, m, j, :, low:high] = piece
                        outgoing[t * per_tile + i, m, j, :, low:high] = piece.astype(BF16)
        made = []
        for k in range(1, lanes):
            there = lax.rem(lane + k, lanes)
            made.append(
                copies.start(
                    outgoing.at[pl.ds(t * per_tile, per_tile), there],
                    landing.at[lane, pl.ds(t * per_tile, per_tile)],
                    plane * row + 2 * there + core,
                )
            )
        lane_copies.append(made)

    sender_core = lax.div(row, half)

    def line_copy(i, j):
        return pltpu.make_async_remote_copy(
            src_ref=forward.at[i, j],
            dst_ref=landed.at[row],
            send_sem=line_send.at[i, j],
            recv_sem=line_recv.at[row],
            device_id=(plane * (half * core + i) + column + j,),
            device_id_type=MESH,
        )

    for t in range(TILES):
        wait_all(lane_copies[t])
        for i in range(t * per_tile, (t + 1) * per_tile):
            for j in range(2):
                total = own[i, lane, j]
                for k in range(1, lanes):
                    total = total + landing[lax.rem(lane + k, lanes), i, j].astype(F32)
                sums[i, j] = total
                forward[i, j] = total.astype(BF16)

                @pl.when(plane * (half * core + i) + column + j != me)
                def _():
                    line_copy(i, j).start()

    for i in range(half):
        for j in range(2):

            @pl.when(plane * (half * core + i) + column + j != me)
            def _():
                line_copy(i, j).wait_send()

    for sender_row in range(rows):
        sender = plane * sender_row + column + sender_core

        @pl.when(sender != me)
        def _():
            pltpu.make_async_remote_copy(
                src_ref=forward.at[0, 0],
                dst_ref=landed.at[sender_row],
                send_sem=line_send.at[0, 0],
                recv_sem=line_recv.at[sender_row],
                device_id=(sender,),
                device_id_type=MESH,
            ).wait_recv()

    total = jnp.where(sender_core == core, sums[lax.rem(row, half), core], 0.0)
    for sender_row in range(rows):
        sender = plane * sender_row + column + sender_core
        total = total + jnp.where(sender == me, 0.0, landed[sender_row].astype(F32))
    out_first[...] = total[:, :width]
    out_second[...] = total[:, width:]


def step(size, plane, score_scale, facts, *arrays):
    query_features, _, _, base_pos, units, w_first, w_second = arrays
    rows, lanes = size // plane, plane // 2
    half = rows // 2
    width, hidden_width = w_first.shape
    embed = w_second.shape[1]
    chunk = hidden_width // size
    across = width + embed
    base, unit = base_pos.shape[1], units.shape[1]
    block = base + unit
    vmem = pl.BlockSpec(memory_space=pltpu.VMEM)
    count = 15 + 4 * (plane - 1) + 2 * (rows - 1) + 2
    count += 2 * (plane - 1) + 3 * (rows - 1) + 2 + TILES * (lanes - 1)

    def split(members, dtype):
        return [
            pltpu.VMEM((members, base, embed), dtype),
            pltpu.VMEM((members, unit, embed), dtype),
        ]

    scratch = [
        pltpu.VMEM((16,) + units.shape[1:], BF16),
        pltpu.VMEM((2, 2, base, width), BF16),
        pltpu.VMEM((2, 2, unit, width), BF16),
        *split(plane, BF16),
        *split(rows, BF16),
        pltpu.VMEM((plane, 2, 1, base), F32),
        pltpu.VMEM((plane * block, embed), BF16),
        pltpu.VMEM((rows * block, embed), BF16),
        pltpu.VMEM((rows * block, plane * block), F32),
        pltpu.VMEM((plane, 4, plane * block), F32),
        *split(plane, F32),
        *split(plane, BF16),
        *split(plane, BF16),
        *split(rows, F32),
        *split(rows, BF16),
        *split(rows, BF16),
        pltpu.VMEM((rows, 8, 128), F32),
        pltpu.VMEM((2, 2, base, embed), BF16),
        pltpu.VMEM((2, 2, unit, embed), BF16),
        pltpu.VMEM((4 * block, width), BF16),
        pltpu.VMEM((half, lanes, 2, chunk, across), F32),
        pltpu.VMEM((half, lanes, 2, chunk, across), BF16),
        pltpu.VMEM((lanes, half, 2, chunk, across), BF16),
        pltpu.VMEM((half, 2, chunk, across), F32),
        pltpu.VMEM((half, 2, chunk, across), BF16),
        pltpu.VMEM((rows, chunk, across), BF16),
        pltpu.SemaphoreType.DMA((count,)),
        pltpu.SemaphoreType.DMA((count,)),
        pltpu.SemaphoreType.DMA((half, 2)),
        pltpu.SemaphoreType.DMA((rows,)),
    ]
    return pl.pallas_call(
        functools.partial(step_kernel, size, plane, score_scale),
        out_shape=[
            jax.ShapeDtypeStruct((8, 128), F32),
            jax.ShapeDtypeStruct((chunk, width), F32),
            jax.ShapeDtypeStruct((chunk, embed), F32),
        ],
        in_specs=[pl.BlockSpec(memory_space=pltpu.SMEM)] + [vmem] * 7,
        out_specs=[vmem] * 3,
        scratch_shapes=scratch,
        compiler_params=pltpu.CompilerParams(
            collective_id=0, has_side_effects=True, vmem_limit_bytes=60 * 1024 * 1024
        ),
    )(facts, *arrays)


def body(query_features, passage_features, counts, positives, w_first, w_second):
    device_count = lax.axis_size("dp")
    plane = 1 << device_count.bit_length() // 2
    rows = device_count // plane
    my_index = lax.axis_index("dp")
    stride = device_count // 16
    base_rows = query_features.shape[0] // 2
    unit_rows = base_rows // 16
    block_rows = base_rows + unit_rows
    pair_count = block_rows * device_count
    score_scale = 2.5 * w_second.shape[1] ** (-0.5)

    devices = jnp.arange(device_count, dtype=jnp.int32)
    heavy_dev = (counts > base_rows).astype(jnp.int32)
    line = my_index % plane + plane * jnp.arange(rows, dtype=jnp.int32)
    asked = jnp.concatenate([my_index[None], line]).astype(jnp.int32)
    same_mat = (devices[None, :] % stride == asked[:, None] % stride) & (heavy_dev[None, :] == 1)
    source = jnp.sum(jnp.where(same_mat, devices[None, :], 0), axis=1)
    offset = jnp.sum(jnp.where(devices[None, :] < asked[:, None], counts[None, :], 0), axis=1)
    source_offset = jnp.sum(
        jnp.where(devices[None, :] < source[:, None], counts[None, :], 0), axis=1
    )
    piece = asked // stride - (source < asked).astype(jnp.int32)
    tail_offset = jnp.where(
        source == asked, offset + base_rows, source_offset + block_rows + piece * unit_rows
    )
    mine = jnp.stack([source[0] // stride, (source[0] == my_index).astype(jnp.int32)])
    facts = jnp.stack([jnp.pad(mine, (0, rows - 2)), offset[1:], tail_offset[1:]])

    lanes = jnp.arange(128, dtype=jnp.int32)
    spare = positives[base_rows:]
    coded = jnp.where(lanes[None, :] == 0, spare[:, None] // 256, spare[:, None] % 256)
    coded = jnp.where(lanes[None, :] < 2, coded, 0).astype(BF16)
    units = jnp.concatenate(
        [query_features[block_rows:], passage_features[block_rows:], coded[unit_rows:]], axis=1
    )
    units = units.reshape(15, unit_rows, units.shape[1])
    losses, total_first, total_second = step(
        device_count,
        plane,
        score_scale,
        facts,
        query_features,
        passage_features,
        coded[:unit_rows],
        positives[:base_rows].astype(F32)[None, :],
        units,
        w_first,
        w_second,
    )
    return (losses[0, 0] / pair_count, total_first.T, total_second)


def solution(mesh):
    return jax.shard_map(
        body,
        mesh=mesh,
        in_specs=(P("dp", None), P("dp", None), P(), P("dp"), P(), P()),
        out_specs=(P(), P(None, "dp"), P("dp", None)),
        check_vma=False,
    )
```

```python
import functools

import jax
import jax.numpy as jnp
from jax import lax
from jax.experimental import pallas as pl
from jax.experimental.pallas import tpu as pltpu
from jax.sharding import PartitionSpec as P

MESH = pl.DeviceIdType.MESH
F32 = jnp.float32
BF16 = jnp.bfloat16
GELU_ROOT = 0.7978845608028654
GELU_CUBE = 0.044715
TILES = 2


def gelu_and_slope(value):
    square = value * value
    bent = jnp.tanh(GELU_ROOT * value * (1.0 + GELU_CUBE * square))
    rise = 0.5 * (1.0 + bent)
    slope = rise + 0.5 * value * (1.0 - bent * bent) * (
        GELU_ROOT * (1.0 + 3.0 * GELU_CUBE * square)
    )
    return value * rise, slope


def dot(left, right, left_dim, right_dim):
    return lax.dot_general(
        left, right, (((left_dim,), (right_dim,)), ((), ())), preferred_element_type=F32
    )


def flat_rows(blocks):
    return blocks.astype(F32).reshape(-1, blocks.shape[-1]).astype(BF16)


class Copies:
    def __init__(self, send, recv):
        self.send, self.recv, self.used = send, recv, 0

    def start(self, source, landing, device):
        copy = pltpu.make_async_remote_copy(
            src_ref=source,
            dst_ref=landing,
            send_sem=self.send.at[self.used],
            recv_sem=self.recv.at[self.used],
            device_id=(device,),
            device_id_type=MESH,
        )
        self.used += 1
        copy.start()
        return copy


def wait_all(copies):
    for copy in copies:
        copy.wait()


def step_kernel(
    size,
    plane,
    score_scale,
    counts,
    query_features,
    passage_features,
    positives,
    w_first,
    w_second,
    out_loss,
    out_all,
    units,
    unit_land,
    unit_pos,
    feat_base,
    feat_tail,
    q_base,
    q_tail,
    p_base,
    p_tail,
    pos_land,
    all_q,
    all_p,
    scores,
    stat_land,
    dq_own_base,
    dq_own_tail,
    dq_out_base,
    dq_out_tail,
    dq_land_base,
    dq_land_tail,
    dp_own_base,
    dp_own_tail,
    dp_out_base,
    dp_out_tail,
    dp_land_base,
    dp_land_tail,
    loss_land,
    de_base,
    de_tail,
    all_x,
    own,
    outgoing,
    landing,
    sums,
    forward,
    landed,
    send_sems,
    recv_sems,
    line_send,
    line_recv,
):
    me = lax.axis_index("dp")
    rows = size // plane
    half = rows // 2
    lanes = plane // 2
    stride = size // 16
    row = lax.div(me, plane)
    spot = lax.rem(me, plane)
    core = lax.rem(me, 2)
    lane = lax.div(spot, 2)
    column = spot - core
    place = lax.div(me, stride)
    partner = me + 1 - 2 * core
    width, hidden_width = w_first.shape
    embed = w_second.shape[1]
    base = q_base.shape[1]
    unit = q_tail.shape[1]
    hidden_half = hidden_width // 2
    tile = hidden_half // TILES
    per_tile = half // TILES
    chunk = hidden_half // (half * lanes * 2)
    copies = Copies(send_sems, recv_sems)

    plane_peers = [row * plane + lax.rem(spot + k, plane) for k in range(1, plane)]
    line_peers = [lax.rem(row + k, rows) * plane + spot for k in range(1, rows)]
    barrier = pltpu.get_barrier_semaphore()

    def greet(device):
        pl.semaphore_signal(barrier, inc=1, device_id=(device,), device_id_type=MESH)

    for k in range(1, 16):
        greet(lax.rem(place + k, 16) * stride + lax.rem(me, stride))
    for device in plane_peers:
        greet(device)
    in_column = 2 * row + core
    for k in range(1, 2 * rows):
        other = lax.rem(in_column + k, 2 * rows)
        greet(plane * lax.div(other, 2) + column + lax.rem(other, 2))
    pl.semaphore_wait(barrier, 15 + plane - 1 + 2 * rows - 1)

    spare = base + unit
    units[:, :, :width] = query_features[spare:].astype(F32).reshape(15, unit, width).astype(BF16)
    units[:, :, width:] = passage_features[spare:].astype(F32).reshape(15, unit, width).astype(BF16)
    unit_pos[place] = positives[...].astype(F32)

    unit_copies = []
    for k in range(1, 16):
        wrap = lax.div(place + k, 16)
        there = place + k - 16 * wrap
        unit_copies.append(
            copies.start(
                units.at[there - 1 + wrap],
                unit_land.at[place],
                there * stride + lax.rem(me, stride),
            )
        )
        unit_copies.append(
            copies.start(
                unit_pos.at[place], unit_pos.at[place], there * stride + lax.rem(me, stride)
            )
        )

    heavies = []
    for g in range(stride):
        at = jnp.int32(0)
        for k in range(16):
            at = at + jnp.where(counts[g + stride * k] > base, g + stride * k, 0)
        heavies.append(at)
    source = jnp.int32(0)
    for g in range(stride):
        source = source + jnp.where(lax.rem(me, stride) == g, heavies[g], 0)
    heavy_place = jnp.int32(0)
    for k in range(16):
        heavy_place = heavy_place + jnp.where(source >= stride * (k + 1), 1, 0)

    def offset_of(device):
        before = jnp.int32(0)
        for at in heavies:
            before = before + jnp.where(at < device, 1, 0)
        return base * (device + before)

    def tail_row(device):
        piece = lax.div(device, stride) - jnp.where(source < device, 1, 0)
        return jnp.where(source == device, base, spare + unit * piece)

    def tower(features):
        total = None
        for low in range(0, hidden_width, tile):
            act = dot(features, w_first[:, low : low + tile], 1, 0)
            hidden = gelu_and_slope(act)[0].astype(BF16)
            part = dot(hidden, w_second[low : low + tile, :], 1, 0)
            total = part if total is None else total + part
        return total.astype(BF16)

    feat_base[core, 0] = query_features[:base]
    feat_base[core, 1] = passage_features[:base]
    pair_x = [copies.start(feat_base.at[core], feat_base.at[core], partner)]
    embedded = tower(feat_base[core].reshape(2 * base, width))
    q_base[spot] = embedded[:base]
    p_base[row] = embedded[base:]
    q_copies = [copies.start(q_base.at[spot], q_base.at[spot], device) for device in plane_peers]
    p_copies = [copies.start(p_base.at[row], p_base.at[row], device) for device in line_peers]

    wait_all(unit_copies)
    heavy = source == me
    got = unit_land[heavy_place].astype(F32)
    tail_q = jnp.where(heavy, query_features[base:spare].astype(F32), got[:, :width])
    tail_p = jnp.where(heavy, passage_features[base:spare].astype(F32), got[:, width:])
    slots = lax.broadcasted_iota(jnp.int32, (unit, positives.shape[1]), 1)
    chosen = lax.broadcasted_iota(jnp.int32, slots.shape, 0) + tail_row(me)
    tail_pos = jnp.sum(
        jnp.where(slots == chosen, unit_pos[heavy_place], 0.0), axis=1, keepdims=True
    )
    tail_x = jnp.concatenate([tail_q, tail_p], axis=0)
    feat_tail[core] = tail_x.reshape(2, unit, width).astype(BF16)
    tail_e = tower(tail_x.astype(BF16)).astype(F32)
    q_tail[spot] = tail_e[:unit].astype(BF16)
    p_tail[row] = tail_e[unit:].astype(BF16)
    pos_land[spot, 0] = positives[:, :base].astype(F32)
    sub = lax.broadcasted_iota(jnp.int32, (unit, base), 0) + spot * unit
    along = lax.broadcasted_iota(jnp.int32, (unit, base), 1)
    pos_land[spot, 1] = jnp.sum(jnp.where(sub == along, tail_pos, 0.0), axis=0, keepdims=True)
    for device in plane_peers:
        q_copies.append(copies.start(pos_land.at[spot], pos_land.at[spot], device))
        q_copies.append(copies.start(q_tail.at[spot], q_tail.at[spot], device))
    for device in line_peers:
        p_copies.append(copies.start(p_tail.at[row], p_tail.at[row], device))
    pair_x.append(copies.start(feat_tail.at[core], feat_tail.at[core], partner))
    wait_all(q_copies)
    wait_all(p_copies)

    q_rows, p_rows = plane * base, rows * base
    all_q[:q_rows] = q_base[...].reshape(q_rows, embed)
    all_q[q_rows:] = flat_rows(q_tail[...])
    all_p[:p_rows] = p_base[...].reshape(p_rows, embed)
    all_p[p_rows:] = flat_rows(p_tail[...])
    pos_tail = pos_land[0, 1]
    for k in range(1, plane):
        pos_tail = pos_tail + pos_land[k, 1]
    wanted = jnp.concatenate(
        [pos_land[k, 0] for k in range(plane)] + [pos_tail[:, : plane * unit]], axis=1
    )
    line = [plane * k + spot for k in range(rows)]
    ids = jnp.concatenate(
        [lax.broadcasted_iota(jnp.int32, (base, 1), 0) + offset_of(device) for device in line]
        + [
            lax.broadcasted_iota(jnp.int32, (unit, 1), 0) + offset_of(source) + tail_row(device)
            for device in line
        ],
        axis=0,
    ).astype(F32)
    scores[...] = score_scale * dot(all_p[...], all_q[...], 1, 1)
    value = scores[...]
    hit = ids == wanted
    top = jnp.max(value, axis=0, keepdims=True)
    stat_land[spot, 0:1] = top
    stat_land[spot, 1:2] = jnp.sum(jnp.exp(value - top), axis=0, keepdims=True)
    stat_land[spot, 2:3] = jnp.sum(jnp.where(hit, value, 0.0), axis=0, keepdims=True)
    stat_land[spot, 3:4] = jnp.zeros_like(top)
    wait_all(
        [copies.start(stat_land.at[spot], stat_land.at[spot], device) for device in plane_peers]
    )
    stats = stat_land[...]
    tops = stats[:, 0]
    row_top = jnp.max(tops, axis=0, keepdims=True)
    mass = jnp.sum(stats[:, 1] * jnp.exp(tops - row_top), axis=0, keepdims=True)
    log_norm = row_top + jnp.log(mass)
    found = jnp.sum(stats[:, 2], axis=0, keepdims=True)
    loss_land[row] = jnp.broadcast_to(
        jnp.sum(log_norm - found, axis=1, keepdims=True), loss_land.shape[1:]
    )
    grads_t = (jnp.exp(scores[...] - log_norm) - hit.astype(F32)).astype(BF16)

    def scatter(part, own_base, own_tail, out_base, out_tail, land_base, land_tail, mine, peers):
        split = own_base.shape[0] * base
        own_base[...] = part[:split].reshape(own_base.shape)
        own_tail[...] = part[split:].reshape(own_tail.shape)
        out_base[...] = own_base[...].astype(out_base.dtype)
        out_tail[...] = own_tail[...].astype(out_tail.dtype)
        made = []
        for there, device in peers:
            made.append(copies.start(out_base.at[there], land_base.at[mine], device))
            made.append(copies.start(out_tail.at[there], land_tail.at[mine], device))
        return made

    def gathered(own_part, land, mine, members):
        total = own_part[mine]
        for k in range(1, members):
            total = total + land[lax.rem(mine + k, members)].astype(F32)
        return total.astype(BF16)

    dq_copies = scatter(
        score_scale * dot(grads_t, all_p[...], 0, 0),
        dq_own_base,
        dq_own_tail,
        dq_out_base,
        dq_out_tail,
        dq_land_base,
        dq_land_tail,
        spot,
        [(lax.rem(spot + k, plane), plane_peers[k - 1]) for k in range(1, plane)],
    )
    dp_copies = scatter(
        score_scale * dot(grads_t, all_q[...], 1, 0),
        dp_own_base,
        dp_own_tail,
        dp_out_base,
        dp_out_tail,
        dp_land_base,
        dp_land_tail,
        row,
        [(lax.rem(row + k, rows), line_peers[k - 1]) for k in range(1, rows)],
    )
    loss_copies = [
        copies.start(loss_land.at[row], loss_land.at[row], device) for device in line_peers
    ]
    wait_all(pair_x)
    x_rows = 4 * base
    all_x[:x_rows] = feat_base[...].reshape(x_rows, width)
    all_x[x_rows:] = flat_rows(feat_tail[...])
    wait_all(dq_copies)
    de_base[core, 0] = gathered(dq_own_base, dq_land_base, spot, plane)
    de_tail[core, 0] = gathered(dq_own_tail, dq_land_tail, spot, plane)
    wait_all(dp_copies)
    de_base[core, 1] = gathered(dp_own_base, dp_land_base, row, rows)
    de_tail[core, 1] = gathered(dp_own_tail, dp_land_tail, row, rows)
    pair_de = [
        copies.start(de_base.at[core], de_base.at[core], partner),
        copies.start(de_tail.at[core], de_tail.at[core], partner),
    ]
    wait_all(loss_copies)
    loss = loss_land[0]
    for k in range(1, rows):
        loss = loss + loss_land[k]
    out_loss[...] = loss * (1.0 / (size * spare))

    lane_copies = []
    for t in range(TILES):
        start = pl.multiple_of(core * hidden_half + t * tile, 128)
        act = dot(all_x[...], w_first[:, pl.ds(start, tile)], 1, 0)
        hidden, slope = gelu_and_slope(act)
        hidden = hidden.astype(BF16)
        if t == 0:
            wait_all(pair_de)
        de = jnp.concatenate(
            [de_base[...].reshape(x_rows, embed), flat_rows(de_tail[...])], axis=0
        )
        back = dot(de, w_second[pl.ds(start, tile), :], 1, 1)
        act_grad = (slope * back).astype(BF16)
        first = dot(act_grad, all_x[...], 0, 0)
        second = dot(hidden, de, 0, 0)
        for i in range(per_tile):
            for m in range(lanes):
                for j in range(2):
                    at = ((i * lanes + m) * 2 + j) * chunk
                    for part, low in ((first, 0), (second, width)):
                        high = low + part.shape[1]
                        piece = part[at : at + chunk]
                        own[t * per_tile + i, m, j, :, low:high] = piece
                        outgoing[t * per_tile + i, m, j, :, low:high] = piece.astype(BF16)
        made = []
        for k in range(1, lanes):
            there = lax.rem(lane + k, lanes)
            made.append(
                copies.start(
                    outgoing.at[pl.ds(t * per_tile, per_tile), there],
                    landing.at[lane, pl.ds(t * per_tile, per_tile)],
                    plane * row + 2 * there + core,
                )
            )
        lane_copies.append(made)

    sender_core = lax.div(row, half)

    def line_copy(i, j):
        return pltpu.make_async_remote_copy(
            src_ref=forward.at[i, j],
            dst_ref=landed.at[row],
            send_sem=line_send.at[i, j],
            recv_sem=line_recv.at[row],
            device_id=(plane * (half * core + i) + column + j,),
            device_id_type=MESH,
        )

    for t in range(TILES):
        wait_all(lane_copies[t])
        for i in range(t * per_tile, (t + 1) * per_tile):
            for j in range(2):
                total = own[i, lane, j]
                for k in range(1, lanes):
                    total = total + landing[lax.rem(lane + k, lanes), i, j].astype(F32)
                sums[i, j] = total
                forward[i, j] = total.astype(BF16)

                @pl.when(plane * (half * core + i) + column + j != me)
                def _():
                    line_copy(i, j).start()

    for i in range(half):
        for j in range(2):

            @pl.when(plane * (half * core + i) + column + j != me)
            def _():
                line_copy(i, j).wait_send()

    for sender_row in range(rows):
        sender = plane * sender_row + column + sender_core

        @pl.when(sender != me)
        def _():
            pltpu.make_async_remote_copy(
                src_ref=forward.at[0, 0],
                dst_ref=landed.at[sender_row],
                send_sem=line_send.at[0, 0],
                recv_sem=line_recv.at[sender_row],
                device_id=(sender,),
                device_id_type=MESH,
            ).wait_recv()

    total = jnp.where(sender_core == core, sums[lax.rem(row, half), core], 0.0)
    for sender_row in range(rows):
        sender = plane * sender_row + column + sender_core
        total = total + jnp.where(sender == me, 0.0, landed[sender_row].astype(F32))
    out_all[...] = total


def split_kernel(loss, total, mean_loss, first, second):
    width = first.shape[1]
    mean_loss[0] = loss[0, 0]
    first[...] = total[:, :width]
    second[...] = total[:, width:]


def split_outputs(loss, total, width):
    vmem = pl.BlockSpec(memory_space=pltpu.VMEM)
    chunk, across = total.shape
    return pl.pallas_call(
        split_kernel,
        out_shape=[
            jax.ShapeDtypeStruct((1,), F32),
            jax.ShapeDtypeStruct((chunk, width), F32),
            jax.ShapeDtypeStruct((chunk, across - width), F32),
        ],
        in_specs=[pl.BlockSpec(memory_space=pltpu.SMEM), vmem],
        out_specs=[pl.BlockSpec(memory_space=pltpu.SMEM), vmem, vmem],
    )(loss, total)


def step(size, plane, score_scale, counts, *arrays):
    query_features, _, positives, w_first, w_second = arrays
    rows, lanes = size // plane, plane // 2
    half = rows // 2
    width, hidden_width = w_first.shape
    embed = w_second.shape[1]
    chunk = hidden_width // size
    across = width + embed
    base = query_features.shape[0] // 2
    unit = base // 16
    block = base + unit
    vmem = pl.BlockSpec(memory_space=pltpu.VMEM)
    count = 30 + 4 * (plane - 1) + 2 * (rows - 1) + 2
    count += 2 * (plane - 1) + 3 * (rows - 1) + 2 + TILES * (lanes - 1)

    def split(members, dtype):
        return [
            pltpu.VMEM((members, base, embed), dtype),
            pltpu.VMEM((members, unit, embed), dtype),
        ]

    scratch = [
        pltpu.VMEM((15, unit, 2 * width), BF16),
        pltpu.VMEM((16, unit, 2 * width), BF16),
        pltpu.VMEM((16,) + positives.shape, F32),
        pltpu.VMEM((2, 2, base, width), BF16),
        pltpu.VMEM((2, 2, unit, width), BF16),
        *split(plane, BF16),
        *split(rows, BF16),
        pltpu.VMEM((plane, 2, 1, base), F32),
        pltpu.VMEM((plane * block, embed), BF16),
        pltpu.VMEM((rows * block, embed), BF16),
        pltpu.VMEM((rows * block, plane * block), F32),
        pltpu.VMEM((plane, 4, plane * block), F32),
        *split(plane, F32),
        *split(plane, BF16),
        *split(plane, BF16),
        *split(rows, F32),
        *split(rows, BF16),
        *split(rows, BF16),
        pltpu.VMEM((rows, 8, 128), F32),
        pltpu.VMEM((2, 2, base, embed), BF16),
        pltpu.VMEM((2, 2, unit, embed), BF16),
        pltpu.VMEM((4 * block, width), BF16),
        pltpu.VMEM((half, lanes, 2, chunk, across), F32),
        pltpu.VMEM((half, lanes, 2, chunk, across), BF16),
        pltpu.VMEM((lanes, half, 2, chunk, across), BF16),
        pltpu.VMEM((half, 2, chunk, across), F32),
        pltpu.VMEM((half, 2, chunk, across), BF16),
        pltpu.VMEM((rows, chunk, across), BF16),
        pltpu.SemaphoreType.DMA((count,)),
        pltpu.SemaphoreType.DMA((count,)),
        pltpu.SemaphoreType.DMA((half, 2)),
        pltpu.SemaphoreType.DMA((rows,)),
    ]
    return pl.pallas_call(
        functools.partial(step_kernel, size, plane, score_scale),
        out_shape=[
            jax.ShapeDtypeStruct((8, 128), F32),
            jax.ShapeDtypeStruct((chunk, across), F32),
        ],
        in_specs=[pl.BlockSpec(memory_space=pltpu.SMEM)] + [vmem] * 5,
        out_specs=[vmem] * 2,
        scratch_shapes=scratch,
        compiler_params=pltpu.CompilerParams(
            collective_id=0, has_side_effects=True, vmem_limit_bytes=60 * 1024 * 1024
        ),
    )(counts, *arrays)


def body(query_features, passage_features, counts, positives, w_first, w_second):
    device_count = lax.axis_size("dp")
    plane = 1 << device_count.bit_length() // 2
    score_scale = 2.5 * w_second.shape[1] ** (-0.5)
    loss, total = step(
        device_count,
        plane,
        score_scale,
        counts,
        query_features,
        passage_features,
        positives[None, :],
        w_first,
        w_second,
    )
    mean_loss, grad_first, grad_second = split_outputs(loss, total, w_first.shape[0])
    return (mean_loss[0], grad_first.T, grad_second)


def solution(mesh):
    return jax.shard_map(
        body,
        mesh=mesh,
        in_specs=(P("dp", None), P("dp", None), P(), P("dp"), P(), P()),
        out_specs=(P(), P(None, "dp"), P("dp", None)),
        check_vma=False,
    )
```

```python
import functools

import jax
import jax.numpy as jnp
from jax import lax
from jax.experimental import pallas as pl
from jax.experimental.pallas import tpu as pltpu
from jax.sharding import PartitionSpec as P

MESH = pl.DeviceIdType.MESH
F32 = jnp.float32
BF16 = jnp.bfloat16
GELU_ROOT = 0.7978845608028654
GELU_CUBE = 0.044715
TILES = 2


def gelu_and_slope(value):
    square = value * value
    bent = jnp.tanh(GELU_ROOT * value * (1.0 + GELU_CUBE * square))
    rise = 0.5 * (1.0 + bent)
    slope = rise + 0.5 * value * (1.0 - bent * bent) * (
        GELU_ROOT * (1.0 + 3.0 * GELU_CUBE * square)
    )
    return value * rise, slope


def dot(left, right, left_dim, right_dim):
    return lax.dot_general(
        left, right, (((left_dim,), (right_dim,)), ((), ())), preferred_element_type=F32
    )


def flat_rows(blocks):
    return blocks.astype(F32).reshape(-1, blocks.shape[-1]).astype(BF16)


class Copies:
    def __init__(self, send, recv):
        self.send, self.recv, self.used = send, recv, 0

    def start(self, source, landing, device):
        copy = pltpu.make_async_remote_copy(
            src_ref=source,
            dst_ref=landing,
            send_sem=self.send.at[self.used],
            recv_sem=self.recv.at[self.used],
            device_id=(device,),
            device_id_type=MESH,
        )
        self.used += 1
        copy.start()
        return copy


def wait_all(copies):
    for copy in copies:
        copy.wait()


def step_kernel(
    size,
    plane,
    score_scale,
    counts,
    query_features,
    passage_features,
    positives,
    w_first_hbm,
    w_second_hbm,
    out_loss,
    out_all,
    units,
    unit_mid,
    unit_pass,
    unit_land,
    unit_pos,
    feat_base,
    feat_tail,
    q_base,
    q_tail,
    p_base,
    p_tail,
    pos_land,
    all_q,
    all_p,
    scores,
    stat_land,
    dq_own_base,
    dq_own_tail,
    dq_out_base,
    dq_out_tail,
    dq_land_base,
    dq_land_tail,
    dp_own_base,
    dp_own_tail,
    dp_out_base,
    dp_out_tail,
    dp_land_base,
    dp_land_tail,
    loss_land,
    de_base,
    de_tail,
    all_x,
    own,
    outgoing,
    landing,
    sums,
    forward,
    landed,
    send_sems,
    recv_sems,
    line_send,
    line_recv,
    w_first,
    w_second,
    all_hidden,
    all_slope,
    load_sems,
):
    me = lax.axis_index("dp")
    loads = [
        pltpu.make_async_copy(w_first_hbm, w_first, load_sems.at[0]),
        pltpu.make_async_copy(w_second_hbm, w_second, load_sems.at[1]),
    ]
    for load in loads:
        load.start()
    rows = size // plane
    half = rows // 2
    lanes = plane // 2
    stride = size // 16
    row = lax.div(me, plane)
    spot = lax.rem(me, plane)
    core = lax.rem(me, 2)
    lane = lax.div(spot, 2)
    column = spot - core
    place = lax.div(me, stride)
    partner = me + 1 - 2 * core
    width, hidden_width = w_first.shape
    embed = w_second.shape[1]
    base = q_base.shape[1]
    unit = q_tail.shape[1]
    hidden_half = hidden_width // 2
    tile = hidden_half // TILES
    per_tile = half // TILES
    chunk = hidden_half // (half * lanes * 2)
    copies = Copies(send_sems, recv_sems)

    plane_peers = [row * plane + lax.rem(spot + k, plane) for k in range(1, plane)]
    line_peers = [lax.rem(row + k, rows) * plane + spot for k in range(1, rows)]
    barrier = pltpu.get_barrier_semaphore()

    def greet(device):
        pl.semaphore_signal(barrier, inc=1, device_id=(device,), device_id_type=MESH)

    for k in range(1, 16):
        greet(lax.rem(place + k, 16) * stride + lax.rem(me, stride))
    for device in plane_peers:
        greet(device)
    in_column = 2 * row + core
    for k in range(1, 2 * rows):
        other = lax.rem(in_column + k, 2 * rows)
        greet(plane * lax.div(other, 2) + column + lax.rem(other, 2))
    pl.semaphore_wait(barrier, 15 + plane - 1 + 2 * rows - 1)

    spare = base + unit
    near = plane // stride
    aside = lax.div(spot, stride)
    extra_q = query_features[spare:].astype(F32).reshape(15, unit, width).astype(BF16)
    extra_p = passage_features[spare:].astype(F32).reshape(15, unit, width).astype(BF16)
    for u in range(15):
        there = u + lax.div(u + 16 - place, 16)
        units[lax.div(there, near), lax.rem(there, near), :, :width] = extra_q[u]
        units[lax.div(there, near), lax.rem(there, near), :, width:] = extra_p[u]
    unit_pos[place] = positives[...].astype(F32)

    mid_copies = []
    for k in range(1, near):
        there = lax.rem(aside + k, near)
        mid_copies.append(
            copies.start(
                units.at[:, there],
                unit_mid.at[aside],
                row * plane + there * stride + lax.rem(me, stride),
            )
        )
    unit_copies = []
    for k in range(1, 16):
        device = lax.rem(place + k, 16) * stride + lax.rem(me, stride)
        unit_copies.append(copies.start(unit_pos.at[place], unit_pos.at[place], device))

    heavies = []
    for g in range(stride):
        at = jnp.int32(0)
        for k in range(16):
            at = at + jnp.where(counts[g + stride * k] > base, g + stride * k, 0)
        heavies.append(at)
    source = jnp.int32(0)
    for g in range(stride):
        source = source + jnp.where(lax.rem(me, stride) == g, heavies[g], 0)
    heavy_place = jnp.int32(0)
    for k in range(16):
        heavy_place = heavy_place + jnp.where(source >= stride * (k + 1), 1, 0)

    def offset_of(device):
        before = jnp.int32(0)
        for at in heavies:
            before = before + jnp.where(at < device, 1, 0)
        return base * (device + before)

    def tail_row(device):
        piece = lax.div(device, stride) - jnp.where(source < device, 1, 0)
        return jnp.where(source == device, base, spare + unit * piece)

    def tower(features):
        total = None
        for low in range(0, hidden_width, tile):
            act = dot(features, w_first[:, low : low + tile], 1, 0)
            hidden = gelu_and_slope(act)[0].astype(BF16)
            part = dot(hidden, w_second[low : low + tile, :], 1, 0)
            total = part if total is None else total + part
        return total.astype(BF16)

    feat_base[core, 0] = query_features[:base]
    feat_base[core, 1] = passage_features[:base]
    pair_x = [copies.start(feat_base.at[core], feat_base.at[core], partner)]
    wait_all(loads)
    embedded = tower(feat_base[core].reshape(2 * base, width))
    q_base[spot] = embedded[:base]
    p_base[row] = embedded[base:]
    q_copies = [copies.start(q_base.at[spot], q_base.at[spot], device) for device in plane_peers]
    wait_all(mid_copies)
    source_row, source_aside = jnp.int32(0), heavy_place
    for k in range(1, rows):
        beyond = heavy_place >= k * near
        source_row = source_row + jnp.where(beyond, 1, 0)
        source_aside = source_aside - jnp.where(beyond, near, 0)
    unit_pass[...] = jnp.where(source_aside == aside, units[:, aside], unit_mid[source_aside])
    for k in range(1, rows):
        there = lax.rem(row + k, rows)
        unit_copies.append(
            copies.start(unit_pass.at[there], unit_land.at[row], there * plane + spot)
        )
    p_copies = [copies.start(p_base.at[row], p_base.at[row], device) for device in line_peers]

    wait_all(unit_copies)
    heavy = source == me
    got = jnp.where(source_row == row, unit_pass[row], unit_land[source_row]).astype(F32)
    tail_q = jnp.where(heavy, query_features[base:spare].astype(F32), got[:, :width])
    tail_p = jnp.where(heavy, passage_features[base:spare].astype(F32), got[:, width:])
    slots = lax.broadcasted_iota(jnp.int32, (unit, positives.shape[1]), 1)
    chosen = lax.broadcasted_iota(jnp.int32, slots.shape, 0) + tail_row(me)
    tail_pos = jnp.sum(
        jnp.where(slots == chosen, unit_pos[heavy_place], 0.0), axis=1, keepdims=True
    )
    tail_x = jnp.concatenate([tail_q, tail_p], axis=0)
    feat_tail[core] = tail_x.reshape(2, unit, width).astype(BF16)
    tail_e = tower(tail_x.astype(BF16)).astype(F32)
    q_tail[spot] = tail_e[:unit].astype(BF16)
    p_tail[row] = tail_e[unit:].astype(BF16)
    pos_land[spot, 0] = positives[:, :base].astype(F32)
    sub = lax.broadcasted_iota(jnp.int32, (unit, base), 0) + spot * unit
    along = lax.broadcasted_iota(jnp.int32, (unit, base), 1)
    pos_land[spot, 1] = jnp.sum(jnp.where(sub == along, tail_pos, 0.0), axis=0, keepdims=True)
    for device in plane_peers:
        q_copies.append(copies.start(pos_land.at[spot], pos_land.at[spot], device))
        q_copies.append(copies.start(q_tail.at[spot], q_tail.at[spot], device))
    for device in line_peers:
        p_copies.append(copies.start(p_tail.at[row], p_tail.at[row], device))
    pair_x.append(copies.start(feat_tail.at[core], feat_tail.at[core], partner))
    wait_all(q_copies)
    wait_all(p_copies)

    q_rows, p_rows = plane * base, rows * base
    all_q[:q_rows] = q_base[...].reshape(q_rows, embed)
    all_q[q_rows:] = flat_rows(q_tail[...])
    all_p[:p_rows] = p_base[...].reshape(p_rows, embed)
    all_p[p_rows:] = flat_rows(p_tail[...])
    pos_tail = pos_land[0, 1]
    for k in range(1, plane):
        pos_tail = pos_tail + pos_land[k, 1]
    wanted = jnp.concatenate(
        [pos_land[k, 0] for k in range(plane)] + [pos_tail[:, : plane * unit]], axis=1
    )
    line = [plane * k + spot for k in range(rows)]
    ids = jnp.concatenate(
        [lax.broadcasted_iota(jnp.int32, (base, 1), 0) + offset_of(device) for device in line]
        + [
            lax.broadcasted_iota(jnp.int32, (unit, 1), 0) + offset_of(source) + tail_row(device)
            for device in line
        ],
        axis=0,
    ).astype(F32)
    scores[...] = score_scale * dot(all_p[...], all_q[...], 1, 1)
    value = scores[...]
    hit = ids == wanted
    top = jnp.max(value, axis=0, keepdims=True)
    stat_land[spot, 0:1] = top
    stat_land[spot, 1:2] = jnp.sum(jnp.exp(value - top), axis=0, keepdims=True)
    stat_land[spot, 2:3] = jnp.sum(jnp.where(hit, value, 0.0), axis=0, keepdims=True)
    stat_land[spot, 3:4] = jnp.zeros_like(top)
    wait_all(
        [copies.start(stat_land.at[spot], stat_land.at[spot], device) for device in plane_peers]
    )
    stats = stat_land[...]
    tops = stats[:, 0]
    row_top = jnp.max(tops, axis=0, keepdims=True)
    mass = jnp.sum(stats[:, 1] * jnp.exp(tops - row_top), axis=0, keepdims=True)
    log_norm = row_top + jnp.log(mass)
    found = jnp.sum(stats[:, 2], axis=0, keepdims=True)
    loss_land[row] = jnp.broadcast_to(
        jnp.sum(log_norm - found, axis=1, keepdims=True), loss_land.shape[1:]
    )
    grads_t = (jnp.exp(scores[...] - log_norm) - hit.astype(F32)).astype(BF16)

    def scatter(part, own_base, own_tail, out_base, out_tail, land_base, land_tail, mine, peers):
        split = own_base.shape[0] * base
        own_base[...] = part[:split].reshape(own_base.shape)
        own_tail[...] = part[split:].reshape(own_tail.shape)
        out_base[...] = own_base[...].astype(out_base.dtype)
        out_tail[...] = own_tail[...].astype(out_tail.dtype)
        made = []
        for there, device in peers:
            made.append(copies.start(out_base.at[there], land_base.at[mine], device))
            made.append(copies.start(out_tail.at[there], land_tail.at[mine], device))
        return made

    def gathered(own_part, land, mine, members):
        total = own_part[mine]
        for k in range(1, members):
            total = total + land[lax.rem(mine + k, members)].astype(F32)
        return total.astype(BF16)

    dq_copies = scatter(
        score_scale * dot(grads_t, all_p[...], 0, 0),
        dq_own_base,
        dq_own_tail,
        dq_out_base,
        dq_out_tail,
        dq_land_base,
        dq_land_tail,
        spot,
        [(lax.rem(spot + k, plane), plane_peers[k - 1]) for k in range(1, plane)],
    )
    dp_copies = scatter(
        score_scale * dot(grads_t, all_q[...], 1, 0),
        dp_own_base,
        dp_own_tail,
        dp_out_base,
        dp_out_tail,
        dp_land_base,
        dp_land_tail,
        row,
        [(lax.rem(row + k, rows), line_peers[k - 1]) for k in range(1, rows)],
    )
    loss_copies = [
        copies.start(loss_land.at[row], loss_land.at[row], device) for device in line_peers
    ]
    wait_all(pair_x)
    x_rows = 4 * base
    all_x[:x_rows] = feat_base[...].reshape(x_rows, width)
    all_x[x_rows:] = flat_rows(feat_tail[...])
    for t in range(TILES):
        start = pl.multiple_of(core * hidden_half + t * tile, 128)
        hidden, slope = gelu_and_slope(dot(all_x[...], w_first[:, pl.ds(start, tile)], 1, 0))
        all_hidden[t] = hidden.astype(BF16)
        all_slope[t] = slope
    wait_all(dq_copies)
    de_base[core, 0] = gathered(dq_own_base, dq_land_base, spot, plane)
    de_tail[core, 0] = gathered(dq_own_tail, dq_land_tail, spot, plane)
    wait_all(dp_copies)
    de_base[core, 1] = gathered(dp_own_base, dp_land_base, row, rows)
    de_tail[core, 1] = gathered(dp_own_tail, dp_land_tail, row, rows)
    pair_de = [
        copies.start(de_base.at[core], de_base.at[core], partner),
        copies.start(de_tail.at[core], de_tail.at[core], partner),
    ]
    wait_all(loss_copies)
    loss = loss_land[0]
    for k in range(1, rows):
        loss = loss + loss_land[k]
    out_loss[...] = loss * (1.0 / (size * spare))

    lane_copies = []
    for t in range(TILES):
        start = pl.multiple_of(core * hidden_half + t * tile, 128)
        if t == 0:
            wait_all(pair_de)
        de = jnp.concatenate(
            [de_base[...].reshape(x_rows, embed), flat_rows(de_tail[...])], axis=0
        )
        back = dot(de, w_second[pl.ds(start, tile), :], 1, 1)
        act_grad = (all_slope[t] * back).astype(BF16)
        first = dot(act_grad, all_x[...], 0, 0)
        second = dot(all_hidden[t], de, 0, 0)
        for i in range(per_tile):
            for m in range(lanes):
                for j in range(2):
                    at = ((i * lanes + m) * 2 + j) * chunk
                    for part, low in ((first, 0), (second, width)):
                        high = low + part.shape[1]
                        piece = part[at : at + chunk]
                        own[t * per_tile + i, m, j, :, low:high] = piece
                        outgoing[t * per_tile + i, m, j, :, low:high] = piece.astype(BF16)
        made = []
        for k in range(1, lanes):
            there = lax.rem(lane + k, lanes)
            made.append(
                copies.start(
                    outgoing.at[pl.ds(t * per_tile, per_tile), there],
                    landing.at[lane, pl.ds(t * per_tile, per_tile)],
                    plane * row + 2 * there + core,
                )
            )
        lane_copies.append(made)

    sender_core = lax.div(row, half)

    def line_copy(i, j):
        return pltpu.make_async_remote_copy(
            src_ref=forward.at[i, j],
            dst_ref=landed.at[row],
            send_sem=line_send.at[i, j],
            recv_sem=line_recv.at[row],
            device_id=(plane * (half * core + i) + column + j,),
            device_id_type=MESH,
        )

    for t in range(TILES):
        wait_all(lane_copies[t])
        for i in range(t * per_tile, (t + 1) * per_tile):
            for j in range(2):
                total = own[i, lane, j]
                for k in range(1, lanes):
                    total = total + landing[lax.rem(lane + k, lanes), i, j].astype(F32)
                sums[i, j] = total
                forward[i, j] = total.astype(BF16)

                @pl.when(plane * (half * core + i) + column + j != me)
                def _():
                    line_copy(i, j).start()

    for i in range(half):
        for j in range(2):

            @pl.when(plane * (half * core + i) + column + j != me)
            def _():
                line_copy(i, j).wait_send()

    for sender_row in range(rows):
        sender = plane * sender_row + column + sender_core

        @pl.when(sender != me)
        def _():
            pltpu.make_async_remote_copy(
                src_ref=forward.at[0, 0],
                dst_ref=landed.at[sender_row],
                send_sem=line_send.at[0, 0],
                recv_sem=line_recv.at[sender_row],
                device_id=(sender,),
                device_id_type=MESH,
            ).wait_recv()

    total = jnp.where(sender_core == core, sums[lax.rem(row, half), core], 0.0)
    for sender_row in range(rows):
        sender = plane * sender_row + column + sender_core
        total = total + jnp.where(sender == me, 0.0, landed[sender_row].astype(F32))
    out_all[...] = total


def split_kernel(loss, total, mean_loss, first, second):
    width = first.shape[1]
    mean_loss[0] = loss[0, 0]
    first[...] = total[:, :width]
    second[...] = total[:, width:]


def split_outputs(loss, total, width):
    vmem = pl.BlockSpec(memory_space=pltpu.VMEM)
    chunk, across = total.shape
    return pl.pallas_call(
        split_kernel,
        out_shape=[
            jax.ShapeDtypeStruct((1,), F32),
            jax.ShapeDtypeStruct((chunk, width), F32),
            jax.ShapeDtypeStruct((chunk, across - width), F32),
        ],
        in_specs=[pl.BlockSpec(memory_space=pltpu.SMEM), vmem],
        out_specs=[pl.BlockSpec(memory_space=pltpu.SMEM), vmem, vmem],
    )(loss, total)


def step(size, plane, score_scale, counts, *arrays):
    query_features, _, positives, w_first, w_second = arrays
    rows, lanes = size // plane, plane // 2
    half = rows // 2
    width, hidden_width = w_first.shape
    embed = w_second.shape[1]
    chunk = hidden_width // size
    across = width + embed
    base = query_features.shape[0] // 2
    unit = base // 16
    block = base + unit
    vmem = pl.BlockSpec(memory_space=pltpu.VMEM)
    count = 30 + 4 * (plane - 1) + 2 * (rows - 1) + 2
    count += 2 * (plane - 1) + 3 * (rows - 1) + 2 + TILES * (lanes - 1)

    def split(members, dtype):
        return [
            pltpu.VMEM((members, base, embed), dtype),
            pltpu.VMEM((members, unit, embed), dtype),
        ]

    scratch = [
        pltpu.VMEM((rows, 16 // rows, unit, 2 * width), BF16),
        pltpu.VMEM((16 // rows, rows, unit, 2 * width), BF16),
        pltpu.VMEM((rows, unit, 2 * width), BF16),
        pltpu.VMEM((rows, unit, 2 * width), BF16),
        pltpu.VMEM((16,) + positives.shape, F32),
        pltpu.VMEM((2, 2, base, width), BF16),
        pltpu.VMEM((2, 2, unit, width), BF16),
        *split(plane, BF16),
        *split(rows, BF16),
        pltpu.VMEM((plane, 2, 1, base), F32),
        pltpu.VMEM((plane * block, embed), BF16),
        pltpu.VMEM((rows * block, embed), BF16),
        pltpu.VMEM((rows * block, plane * block), F32),
        pltpu.VMEM((plane, 4, plane * block), F32),
        *split(plane, F32),
        *split(plane, BF16),
        *split(plane, BF16),
        *split(rows, F32),
        *split(rows, BF16),
        *split(rows, BF16),
        pltpu.VMEM((rows, 8, 128), F32),
        pltpu.VMEM((2, 2, base, embed), BF16),
        pltpu.VMEM((2, 2, unit, embed), BF16),
        pltpu.VMEM((4 * block, width), BF16),
        pltpu.VMEM((half, lanes, 2, chunk, across), F32),
        pltpu.VMEM((half, lanes, 2, chunk, across), BF16),
        pltpu.VMEM((lanes, half, 2, chunk, across), BF16),
        pltpu.VMEM((half, 2, chunk, across), F32),
        pltpu.VMEM((half, 2, chunk, across), BF16),
        pltpu.VMEM((rows, chunk, across), BF16),
        pltpu.SemaphoreType.DMA((count,)),
        pltpu.SemaphoreType.DMA((count,)),
        pltpu.SemaphoreType.DMA((half, 2)),
        pltpu.SemaphoreType.DMA((rows,)),
        pltpu.VMEM(w_first.shape, BF16),
        pltpu.VMEM(w_second.shape, BF16),
        pltpu.VMEM((TILES, 4 * block, hidden_width // 2 // TILES), BF16),
        pltpu.VMEM((TILES, 4 * block, hidden_width // 2 // TILES), F32),
        pltpu.SemaphoreType.DMA((2,)),
    ]
    return pl.pallas_call(
        functools.partial(step_kernel, size, plane, score_scale),
        out_shape=[
            jax.ShapeDtypeStruct((8, 128), F32),
            jax.ShapeDtypeStruct((chunk, across), F32),
        ],
        in_specs=[pl.BlockSpec(memory_space=pltpu.SMEM)] + [vmem] * 3
        + [pl.BlockSpec(memory_space=pl.ANY)] * 2,
        out_specs=[vmem] * 2,
        scratch_shapes=scratch,
        compiler_params=pltpu.CompilerParams(
            collective_id=0, has_side_effects=True, vmem_limit_bytes=60 * 1024 * 1024
        ),
    )(counts, *arrays)


def body(query_features, passage_features, counts, positives, w_first, w_second):
    device_count = lax.axis_size("dp")
    plane = 1 << device_count.bit_length() // 2
    score_scale = 2.5 * w_second.shape[1] ** (-0.5)
    loss, total = step(
        device_count,
        plane,
        score_scale,
        counts,
        query_features,
        passage_features,
        positives[None, :],
        w_first,
        w_second,
    )
    mean_loss, grad_first, grad_second = split_outputs(loss, total, w_first.shape[0])
    return (mean_loss[0], grad_first.T, grad_second)


def solution(mesh):
    return jax.shard_map(
        body,
        mesh=mesh,
        in_specs=(P("dp", None), P("dp", None), P(), P("dp"), P(), P()),
        out_specs=(P(), P(None, "dp"), P("dp", None)),
        check_vma=False,
    )
```

```python
import functools

import jax
import jax.numpy as jnp
from jax import lax
from jax.experimental import pallas as pl
from jax.experimental.pallas import tpu as pltpu
from jax.sharding import PartitionSpec as P

MESH = pl.DeviceIdType.MESH
F32 = jnp.float32
BF16 = jnp.bfloat16
GELU_ROOT = 0.7978845608028654
GELU_CUBE = 0.044715
TILES = 2


def gelu_and_slope(value):
    square = value * value
    bent = jnp.tanh(GELU_ROOT * value * (1.0 + GELU_CUBE * square))
    rise = 0.5 * (1.0 + bent)
    slope = rise + 0.5 * value * (1.0 - bent * bent) * (
        GELU_ROOT * (1.0 + 3.0 * GELU_CUBE * square)
    )
    return value * rise, slope


def dot(left, right, left_dim, right_dim):
    return lax.dot_general(
        left, right, (((left_dim,), (right_dim,)), ((), ())), preferred_element_type=F32
    )


def flat_rows(blocks):
    return blocks.astype(F32).reshape(-1, blocks.shape[-1]).astype(BF16)


class Copies:
    def __init__(self, send, recv):
        self.send, self.recv, self.used = send, recv, 0

    def start(self, source, landing, device):
        copy = pltpu.make_async_remote_copy(
            src_ref=source,
            dst_ref=landing,
            send_sem=self.send.at[self.used],
            recv_sem=self.recv.at[self.used],
            device_id=(device,),
            device_id_type=MESH,
        )
        self.used += 1
        copy.start()
        return copy


def wait_all(copies):
    for copy in copies:
        copy.wait()


def step_kernel(
    size,
    plane,
    score_scale,
    counts,
    query_features,
    passage_features,
    positives,
    w_first_hbm,
    w_second_hbm,
    out_loss,
    out_all,
    units,
    unit_mid,
    unit_pass,
    unit_land,
    unit_pos,
    feat_base,
    feat_tail,
    q_base,
    q_tail,
    p_base,
    p_tail,
    pos_land,
    all_q,
    all_p,
    scores,
    stat_land,
    dq_own_base,
    dq_own_tail,
    dq_out_base,
    dq_out_tail,
    dq_land_base,
    dq_land_tail,
    dp_own_base,
    dp_own_tail,
    dp_out_base,
    dp_out_tail,
    dp_land_base,
    dp_land_tail,
    loss_land,
    de_base,
    de_tail,
    all_x,
    own,
    outgoing,
    landing,
    sums,
    forward,
    landed,
    send_sems,
    recv_sems,
    line_send,
    line_recv,
    w_first,
    w_second,
    all_hidden,
    all_slope,
    load_sems,
):
    me = lax.axis_index("dp")
    loads = [
        pltpu.make_async_copy(w_first_hbm, w_first, load_sems.at[0]),
        pltpu.make_async_copy(w_second_hbm, w_second, load_sems.at[1]),
    ]
    for load in loads:
        load.start()
    rows = size // plane
    half = rows // 2
    lanes = plane // 2
    stride = size // 16
    row = lax.div(me, plane)
    spot = lax.rem(me, plane)
    core = lax.rem(me, 2)
    lane = lax.div(spot, 2)
    column = spot - core
    place = lax.div(me, stride)
    partner = me + 1 - 2 * core
    width, hidden_width = w_first.shape
    embed = w_second.shape[1]
    base = q_base.shape[1]
    unit = q_tail.shape[1]
    hidden_half = hidden_width // 2
    tile = hidden_half // TILES
    per_tile = half // TILES
    chunk = hidden_half // (half * lanes * 2)
    copies = Copies(send_sems, recv_sems)

    plane_peers = [row * plane + lax.rem(spot + k, plane) for k in range(1, plane)]
    line_peers = [lax.rem(row + k, rows) * plane + spot for k in range(1, rows)]
    barrier = pltpu.get_barrier_semaphore()

    def greet(device):
        pl.semaphore_signal(barrier, inc=1, device_id=(device,), device_id_type=MESH)

    for k in range(1, 16):
        greet(lax.rem(place + k, 16) * stride + lax.rem(me, stride))
    for device in plane_peers:
        greet(device)
    in_column = 2 * row + core
    for k in range(1, 2 * rows):
        other = lax.rem(in_column + k, 2 * rows)
        greet(plane * lax.div(other, 2) + column + lax.rem(other, 2))

    spare = base + unit
    near = plane // stride
    aside = lax.div(spot, stride)
    extra_q = query_features[spare:].astype(F32).reshape(15, unit, width).astype(BF16)
    extra_p = passage_features[spare:].astype(F32).reshape(15, unit, width).astype(BF16)
    for u in range(15):
        there = u + lax.div(u + 16 - place, 16)
        units[lax.div(there, near), lax.rem(there, near), :, :width] = extra_q[u]
        units[lax.div(there, near), lax.rem(there, near), :, width:] = extra_p[u]
    unit_pos[place] = positives[...].astype(F32)

    pl.semaphore_wait(barrier, 15 + plane - 1 + 2 * rows - 1)

    mid_copies = []
    for k in range(1, near):
        there = lax.rem(aside + k, near)
        mid_copies.append(
            copies.start(
                units.at[:, there],
                unit_mid.at[aside],
                row * plane + there * stride + lax.rem(me, stride),
            )
        )
    unit_copies = []
    for k in range(1, 16):
        device = lax.rem(place + k, 16) * stride + lax.rem(me, stride)
        unit_copies.append(copies.start(unit_pos.at[place], unit_pos.at[place], device))

    heavies = []
    for g in range(stride):
        at = jnp.int32(0)
        for k in range(16):
            at = at + jnp.where(counts[g + stride * k] > base, g + stride * k, 0)
        heavies.append(at)
    source = jnp.int32(0)
    for g in range(stride):
        source = source + jnp.where(lax.rem(me, stride) == g, heavies[g], 0)
    heavy_place = jnp.int32(0)
    for k in range(16):
        heavy_place = heavy_place + jnp.where(source >= stride * (k + 1), 1, 0)

    def offset_of(device):
        before = jnp.int32(0)
        for at in heavies:
            before = before + jnp.where(at < device, 1, 0)
        return base * (device + before)

    def tail_row(device):
        piece = lax.div(device, stride) - jnp.where(source < device, 1, 0)
        return jnp.where(source == device, base, spare + unit * piece)

    def tower(features):
        total = None
        for low in range(0, hidden_width, tile):
            act = dot(features, w_first[:, low : low + tile], 1, 0)
            hidden = gelu_and_slope(act)[0].astype(BF16)
            part = dot(hidden, w_second[low : low + tile, :], 1, 0)
            total = part if total is None else total + part
        return total.astype(BF16)

    feat_base[core, 0] = query_features[:base]
    feat_base[core, 1] = passage_features[:base]
    pair_x = [copies.start(feat_base.at[core], feat_base.at[core], partner)]
    wait_all(loads)
    embedded = tower(feat_base[core].reshape(2 * base, width))
    q_base[spot] = embedded[:base]
    p_base[row] = embedded[base:]
    q_copies = [copies.start(q_base.at[spot], q_base.at[spot], device) for device in plane_peers]
    wait_all(mid_copies)
    source_row, source_aside = jnp.int32(0), heavy_place
    for k in range(1, rows):
        beyond = heavy_place >= k * near
        source_row = source_row + jnp.where(beyond, 1, 0)
        source_aside = source_aside - jnp.where(beyond, near, 0)
    unit_pass[...] = jnp.where(source_aside == aside, units[:, aside], unit_mid[source_aside])
    for k in range(1, rows):
        there = lax.rem(row + k, rows)
        unit_copies.append(
            copies.start(unit_pass.at[there], unit_land.at[row], there * plane + spot)
        )
    p_copies = [copies.start(p_base.at[row], p_base.at[row], device) for device in line_peers]

    wait_all(unit_copies)
    heavy = source == me
    got = jnp.where(source_row == row, unit_pass[row], unit_land[source_row]).astype(F32)
    tail_q = jnp.where(heavy, query_features[base:spare].astype(F32), got[:, :width])
    tail_p = jnp.where(heavy, passage_features[base:spare].astype(F32), got[:, width:])
    slots = lax.broadcasted_iota(jnp.int32, (unit, positives.shape[1]), 1)
    chosen = lax.broadcasted_iota(jnp.int32, slots.shape, 0) + tail_row(me)
    tail_pos = jnp.sum(
        jnp.where(slots == chosen, unit_pos[heavy_place], 0.0), axis=1, keepdims=True
    )
    tail_x = jnp.concatenate([tail_q, tail_p], axis=0)
    feat_tail[core] = tail_x.reshape(2, unit, width).astype(BF16)
    tail_e = tower(tail_x.astype(BF16)).astype(F32)
    q_tail[spot] = tail_e[:unit].astype(BF16)
    p_tail[row] = tail_e[unit:].astype(BF16)
    pos_land[spot, 0] = positives[:, :base].astype(F32)
    sub = lax.broadcasted_iota(jnp.int32, (unit, base), 0) + spot * unit
    along = lax.broadcasted_iota(jnp.int32, (unit, base), 1)
    pos_land[spot, 1] = jnp.sum(jnp.where(sub == along, tail_pos, 0.0), axis=0, keepdims=True)
    for device in plane_peers:
        q_copies.append(copies.start(pos_land.at[spot], pos_land.at[spot], device))
        q_copies.append(copies.start(q_tail.at[spot], q_tail.at[spot], device))
    for device in line_peers:
        p_copies.append(copies.start(p_tail.at[row], p_tail.at[row], device))
    pair_x.append(copies.start(feat_tail.at[core], feat_tail.at[core], partner))
    wait_all(q_copies)
    wait_all(p_copies)

    q_rows, p_rows = plane * base, rows * base
    all_q[:q_rows] = q_base[...].reshape(q_rows, embed)
    all_q[q_rows:] = flat_rows(q_tail[...])
    all_p[:p_rows] = p_base[...].reshape(p_rows, embed)
    all_p[p_rows:] = flat_rows(p_tail[...])
    pos_tail = pos_land[0, 1]
    for k in range(1, plane):
        pos_tail = pos_tail + pos_land[k, 1]
    wanted = jnp.concatenate(
        [pos_land[k, 0] for k in range(plane)] + [pos_tail[:, : plane * unit]], axis=1
    )
    line = [plane * k + spot for k in range(rows)]
    ids = jnp.concatenate(
        [lax.broadcasted_iota(jnp.int32, (base, 1), 0) + offset_of(device) for device in line]
        + [
            lax.broadcasted_iota(jnp.int32, (unit, 1), 0) + offset_of(source) + tail_row(device)
            for device in line
        ],
        axis=0,
    ).astype(F32)
    scores[...] = score_scale * dot(all_p[...], all_q[...], 1, 1)
    value = scores[...]
    hit = ids == wanted
    top = jnp.max(value, axis=0, keepdims=True)
    stat_land[spot, 0:1] = top
    stat_land[spot, 1:2] = jnp.sum(jnp.exp(value - top), axis=0, keepdims=True)
    stat_land[spot, 2:3] = jnp.sum(jnp.where(hit, value, 0.0), axis=0, keepdims=True)
    stat_land[spot, 3:4] = jnp.zeros_like(top)
    wait_all(
        [copies.start(stat_land.at[spot], stat_land.at[spot], device) for device in plane_peers]
    )
    stats = stat_land[...]
    tops = stats[:, 0]
    row_top = jnp.max(tops, axis=0, keepdims=True)
    mass = jnp.sum(stats[:, 1] * jnp.exp(tops - row_top), axis=0, keepdims=True)
    log_norm = row_top + jnp.log(mass)
    found = jnp.sum(stats[:, 2], axis=0, keepdims=True)
    loss_land[row] = jnp.broadcast_to(
        jnp.sum(log_norm - found, axis=1, keepdims=True), loss_land.shape[1:]
    )
    grads_t = (jnp.exp(scores[...] - log_norm) - hit.astype(F32)).astype(BF16)

    def scatter(part, own_base, own_tail, out_base, out_tail, land_base, land_tail, mine, peers):
        split = own_base.shape[0] * base
        own_base[...] = part[:split].reshape(own_base.shape)
        own_tail[...] = part[split:].reshape(own_tail.shape)
        out_base[...] = own_base[...].astype(out_base.dtype)
        out_tail[...] = own_tail[...].astype(out_tail.dtype)
        made = []
        for there, device in peers:
            made.append(copies.start(out_base.at[there], land_base.at[mine], device))
            made.append(copies.start(out_tail.at[there], land_tail.at[mine], device))
        return made

    def gathered(own_part, land, mine, members):
        total = own_part[mine]
        for k in range(1, members):
            total = total + land[lax.rem(mine + k, members)].astype(F32)
        return total.astype(BF16)

    dq_copies = scatter(
        score_scale * dot(grads_t, all_p[...], 0, 0),
        dq_own_base,
        dq_own_tail,
        dq_out_base,
        dq_out_tail,
        dq_land_base,
        dq_land_tail,
        spot,
        [(lax.rem(spot + k, plane), plane_peers[k - 1]) for k in range(1, plane)],
    )
    dp_copies = scatter(
        score_scale * dot(grads_t, all_q[...], 1, 0),
        dp_own_base,
        dp_own_tail,
        dp_out_base,
        dp_out_tail,
        dp_land_base,
        dp_land_tail,
        row,
        [(lax.rem(row + k, rows), line_peers[k - 1]) for k in range(1, rows)],
    )
    loss_copies = [
        copies.start(loss_land.at[row], loss_land.at[row], device) for device in line_peers
    ]
    wait_all(pair_x)
    x_rows = 4 * base
    all_x[:x_rows] = feat_base[...].reshape(x_rows, width)
    all_x[x_rows:] = flat_rows(feat_tail[...])
    for t in range(TILES):
        start = pl.multiple_of(core * hidden_half + t * tile, 128)
        hidden, slope = gelu_and_slope(dot(all_x[...], w_first[:, pl.ds(start, tile)], 1, 0))
        all_hidden[t] = hidden.astype(BF16)
        all_slope[t] = slope
    wait_all(dq_copies)
    de_base[core, 0] = gathered(dq_own_base, dq_land_base, spot, plane)
    de_tail[core, 0] = gathered(dq_own_tail, dq_land_tail, spot, plane)
    wait_all(dp_copies)
    de_base[core, 1] = gathered(dp_own_base, dp_land_base, row, rows)
    de_tail[core, 1] = gathered(dp_own_tail, dp_land_tail, row, rows)
    pair_de = [
        copies.start(de_base.at[core], de_base.at[core], partner),
        copies.start(de_tail.at[core], de_tail.at[core], partner),
    ]
    wait_all(loss_copies)
    loss = loss_land[0]
    for k in range(1, rows):
        loss = loss + loss_land[k]
    out_loss[...] = loss * (1.0 / (size * spare))

    def keep(t, part, low):
        high = low + part.shape[1]
        for i in range(per_tile):
            for m in range(lanes):
                for j in range(2):
                    at = ((i * lanes + m) * 2 + j) * chunk
                    piece = part[at : at + chunk]
                    own[t * per_tile + i, m, j, :, low:high] = piece
                    outgoing[t * per_tile + i, m, j, :, low:high] = piece.astype(BF16)
        made = []
        block = pl.ds(t * per_tile, per_tile)
        for k in range(1, lanes):
            there = lax.rem(lane + k, lanes)
            made.append(
                copies.start(
                    outgoing.at[block, there, :, :, pl.ds(low, high - low)],
                    landing.at[lane, block, :, :, pl.ds(low, high - low)],
                    plane * row + 2 * there + core,
                )
            )
        return made

    wait_all(pair_de)
    de = jnp.concatenate([de_base[...].reshape(x_rows, embed), flat_rows(de_tail[...])], axis=0)
    lane_copies = [keep(0, dot(all_hidden[0], de, 0, 0), width)]
    for t in range(TILES):
        start = pl.multiple_of(core * hidden_half + t * tile, 128)
        back = dot(de, w_second[pl.ds(start, tile), :], 1, 1)
        act_grad = (all_slope[t] * back).astype(BF16)
        lane_copies[t] += keep(t, dot(act_grad, all_x[...], 0, 0), 0)
        if t + 1 < TILES:
            lane_copies.append(keep(t + 1, dot(all_hidden[t + 1], de, 0, 0), width))

    sender_core = lax.div(row, half)

    def line_copy(i, j):
        return pltpu.make_async_remote_copy(
            src_ref=forward.at[i, j],
            dst_ref=landed.at[row],
            send_sem=line_send.at[i, j],
            recv_sem=line_recv.at[row],
            device_id=(plane * (half * core + i) + column + j,),
            device_id_type=MESH,
        )

    for t in range(TILES):
        wait_all(lane_copies[t])
        for i in range(t * per_tile, (t + 1) * per_tile):
            for j in range(2):
                total = own[i, lane, j]
                for k in range(1, lanes):
                    total = total + landing[lax.rem(lane + k, lanes), i, j].astype(F32)
                sums[i, j] = total
                forward[i, j] = total.astype(BF16)

                @pl.when(plane * (half * core + i) + column + j != me)
                def _():
                    line_copy(i, j).start()

    for i in range(half):
        for j in range(2):

            @pl.when(plane * (half * core + i) + column + j != me)
            def _():
                line_copy(i, j).wait_send()

    for sender_row in range(rows):
        sender = plane * sender_row + column + sender_core

        @pl.when(sender != me)
        def _():
            pltpu.make_async_remote_copy(
                src_ref=forward.at[0, 0],
                dst_ref=landed.at[sender_row],
                send_sem=line_send.at[0, 0],
                recv_sem=line_recv.at[sender_row],
                device_id=(sender,),
                device_id_type=MESH,
            ).wait_recv()

    total = jnp.where(sender_core == core, sums[lax.rem(row, half), core], 0.0)
    for sender_row in range(rows):
        sender = plane * sender_row + column + sender_core
        total = total + jnp.where(sender == me, 0.0, landed[sender_row].astype(F32))
    out_all[...] = total


def split_kernel(loss, total, mean_loss, first, second):
    width = first.shape[1]
    mean_loss[0] = loss[0, 0]
    first[...] = total[:, :width]
    second[...] = total[:, width:]


def split_outputs(loss, total, width):
    vmem = pl.BlockSpec(memory_space=pltpu.VMEM)
    chunk, across = total.shape
    return pl.pallas_call(
        split_kernel,
        out_shape=[
            jax.ShapeDtypeStruct((1,), F32),
            jax.ShapeDtypeStruct((chunk, width), F32),
            jax.ShapeDtypeStruct((chunk, across - width), F32),
        ],
        in_specs=[pl.BlockSpec(memory_space=pltpu.SMEM), vmem],
        out_specs=[pl.BlockSpec(memory_space=pltpu.SMEM), vmem, vmem],
    )(loss, total)


def step(size, plane, score_scale, counts, *arrays):
    query_features, _, positives, w_first, w_second = arrays
    rows, lanes = size // plane, plane // 2
    half = rows // 2
    width, hidden_width = w_first.shape
    embed = w_second.shape[1]
    chunk = hidden_width // size
    across = width + embed
    base = query_features.shape[0] // 2
    unit = base // 16
    block = base + unit
    vmem = pl.BlockSpec(memory_space=pltpu.VMEM)
    count = 30 + 4 * (plane - 1) + 2 * (rows - 1) + 2
    count += 2 * (plane - 1) + 3 * (rows - 1) + 2 + 2 * TILES * (lanes - 1)

    def split(members, dtype):
        return [
            pltpu.VMEM((members, base, embed), dtype),
            pltpu.VMEM((members, unit, embed), dtype),
        ]

    scratch = [
        pltpu.VMEM((rows, 16 // rows, unit, 2 * width), BF16),
        pltpu.VMEM((16 // rows, rows, unit, 2 * width), BF16),
        pltpu.VMEM((rows, unit, 2 * width), BF16),
        pltpu.VMEM((rows, unit, 2 * width), BF16),
        pltpu.VMEM((16,) + positives.shape, F32),
        pltpu.VMEM((2, 2, base, width), BF16),
        pltpu.VMEM((2, 2, unit, width), BF16),
        *split(plane, BF16),
        *split(rows, BF16),
        pltpu.VMEM((plane, 2, 1, base), F32),
        pltpu.VMEM((plane * block, embed), BF16),
        pltpu.VMEM((rows * block, embed), BF16),
        pltpu.VMEM((rows * block, plane * block), F32),
        pltpu.VMEM((plane, 4, plane * block), F32),
        *split(plane, F32),
        *split(plane, BF16),
        *split(plane, BF16),
        *split(rows, F32),
        *split(rows, BF16),
        *split(rows, BF16),
        pltpu.VMEM((rows, 8, 128), F32),
        pltpu.VMEM((2, 2, base, embed), BF16),
        pltpu.VMEM((2, 2, unit, embed), BF16),
        pltpu.VMEM((4 * block, width), BF16),
        pltpu.VMEM((half, lanes, 2, chunk, across), F32),
        pltpu.VMEM((half, lanes, 2, chunk, across), BF16),
        pltpu.VMEM((lanes, half, 2, chunk, across), BF16),
        pltpu.VMEM((half, 2, chunk, across), F32),
        pltpu.VMEM((half, 2, chunk, across), BF16),
        pltpu.VMEM((rows, chunk, across), BF16),
        pltpu.SemaphoreType.DMA((count,)),
        pltpu.SemaphoreType.DMA((count,)),
        pltpu.SemaphoreType.DMA((half, 2)),
        pltpu.SemaphoreType.DMA((rows,)),
        pltpu.VMEM(w_first.shape, BF16),
        pltpu.VMEM(w_second.shape, BF16),
        pltpu.VMEM((TILES, 4 * block, hidden_width // 2 // TILES), BF16),
        pltpu.VMEM((TILES, 4 * block, hidden_width // 2 // TILES), F32),
        pltpu.SemaphoreType.DMA((2,)),
    ]
    return pl.pallas_call(
        functools.partial(step_kernel, size, plane, score_scale),
        out_shape=[
            jax.ShapeDtypeStruct((8, 128), F32),
            jax.ShapeDtypeStruct((chunk, across), F32),
        ],
        in_specs=[pl.BlockSpec(memory_space=pltpu.SMEM)] + [vmem] * 3
        + [pl.BlockSpec(memory_space=pl.ANY)] * 2,
        out_specs=[vmem] * 2,
        scratch_shapes=scratch,
        compiler_params=pltpu.CompilerParams(
            collective_id=0, has_side_effects=True, vmem_limit_bytes=60 * 1024 * 1024
        ),
    )(counts, *arrays)


def body(query_features, passage_features, counts, positives, w_first, w_second):
    device_count = lax.axis_size("dp")
    plane = 1 << device_count.bit_length() // 2
    score_scale = 2.5 * w_second.shape[1] ** (-0.5)
    loss, total = step(
        device_count,
        plane,
        score_scale,
        counts,
        query_features,
        passage_features,
        positives[None, :],
        w_first,
        w_second,
    )
    mean_loss, grad_first, grad_second = split_outputs(loss, total, w_first.shape[0])
    return (mean_loss[0], grad_first.T, grad_second)


def solution(mesh):
    return jax.shard_map(
        body,
        mesh=mesh,
        in_specs=(P("dp", None), P("dp", None), P(), P("dp"), P(), P()),
        out_specs=(P(), P(None, "dp"), P("dp", None)),
        check_vma=False,
    )
```

```python
import functools

import jax
import jax.numpy as jnp
from jax import lax
from jax.experimental import pallas as pl
from jax.experimental.pallas import tpu as pltpu
from jax.sharding import PartitionSpec as P

MESH = pl.DeviceIdType.MESH
F32 = jnp.float32
BF16 = jnp.bfloat16
GELU_ROOT = 0.7978845608028654
GELU_CUBE = 0.044715
TILES = 2


def gelu_and_slope(value):
    square = value * value
    bent = jnp.tanh(GELU_ROOT * value * (1.0 + GELU_CUBE * square))
    rise = 0.5 * (1.0 + bent)
    slope = rise + 0.5 * value * (1.0 - bent * bent) * (
        GELU_ROOT * (1.0 + 3.0 * GELU_CUBE * square)
    )
    return value * rise, slope


def dot(left, right, left_dim, right_dim):
    return lax.dot_general(
        left, right, (((left_dim,), (right_dim,)), ((), ())), preferred_element_type=F32
    )


def flat_rows(blocks):
    return blocks.astype(F32).reshape(-1, blocks.shape[-1]).astype(BF16)


class Copies:
    def __init__(self, send, recv):
        self.send, self.recv, self.used = send, recv, 0

    def start(self, source, landing, device):
        copy = pltpu.make_async_remote_copy(
            src_ref=source,
            dst_ref=landing,
            send_sem=self.send.at[self.used],
            recv_sem=self.recv.at[self.used],
            device_id=(device,),
            device_id_type=MESH,
        )
        self.used += 1
        copy.start()
        return copy


def wait_all(copies):
    for copy in copies:
        copy.wait()


def step_kernel(
    size,
    plane,
    score_scale,
    counts,
    query_features,
    passage_features,
    positives,
    w_first_hbm,
    w_second_hbm,
    out_loss,
    out_all,
    units,
    unit_mid,
    unit_pass,
    unit_land,
    unit_pos,
    feat_base,
    feat_tail,
    q_base,
    q_tail,
    p_base,
    p_tail,
    pos_land,
    all_q,
    all_p,
    scores,
    stat_land,
    dq_own_base,
    dq_own_tail,
    dq_out_base,
    dq_out_tail,
    dq_land_base,
    dq_land_tail,
    dp_own_base,
    dp_own_tail,
    dp_out_base,
    dp_out_tail,
    dp_land_base,
    dp_land_tail,
    loss_land,
    de_base,
    de_tail,
    all_x,
    own,
    outgoing,
    landing,
    sums,
    forward,
    landed,
    send_sems,
    recv_sems,
    line_send,
    line_recv,
    w_first,
    w_second,
    all_hidden,
    all_slope,
    load_sems,
):
    me = lax.axis_index("dp")
    loads = [
        pltpu.make_async_copy(w_first_hbm, w_first, load_sems.at[0]),
        pltpu.make_async_copy(w_second_hbm, w_second, load_sems.at[1]),
    ]
    for load in loads:
        load.start()
    rows = size // plane
    half = rows // 2
    lanes = plane // 2
    stride = size // 16
    row = lax.div(me, plane)
    spot = lax.rem(me, plane)
    core = lax.rem(me, 2)
    lane = lax.div(spot, 2)
    column = spot - core
    place = lax.div(me, stride)
    partner = me + 1 - 2 * core
    width, hidden_width = w_first.shape
    embed = w_second.shape[1]
    base = q_base.shape[1]
    unit = q_tail.shape[1]
    hidden_half = hidden_width // 2
    tile = hidden_half // TILES
    per_tile = half // TILES
    chunk = hidden_half // (half * lanes * 2)
    copies = Copies(send_sems, recv_sems)

    plane_peers = [row * plane + lax.rem(spot + k, plane) for k in range(1, plane)]
    line_peers = [lax.rem(row + k, rows) * plane + spot for k in range(1, rows)]
    barrier = pltpu.get_barrier_semaphore()

    def greet(device):
        pl.semaphore_signal(barrier, inc=1, device_id=(device,), device_id_type=MESH)

    for k in range(1, 16):
        greet(lax.rem(place + k, 16) * stride + lax.rem(me, stride))
    for device in plane_peers:
        greet(device)
    in_column = 2 * row + core
    for k in range(1, 2 * rows):
        other = lax.rem(in_column + k, 2 * rows)
        greet(plane * lax.div(other, 2) + column + lax.rem(other, 2))

    spare = base + unit
    near = plane // stride
    aside = lax.div(spot, stride)
    extra_q = query_features[spare:].astype(F32).reshape(15, unit, width).astype(BF16)
    extra_p = passage_features[spare:].astype(F32).reshape(15, unit, width).astype(BF16)
    for u in range(15):
        there = u + lax.div(u + 16 - place, 16)
        units[lax.div(there, near), lax.rem(there, near), :, :width] = extra_q[u]
        units[lax.div(there, near), lax.rem(there, near), :, width:] = extra_p[u]
    unit_pos[place] = positives[...].astype(F32)

    pl.semaphore_wait(barrier, 15 + plane - 1 + 2 * rows - 1)

    mid_copies = []
    for k in range(1, near):
        there = lax.rem(aside + k, near)
        mid_copies.append(
            copies.start(
                units.at[:, there],
                unit_mid.at[aside],
                row * plane + there * stride + lax.rem(me, stride),
            )
        )
    unit_copies = []
    for k in range(1, 16):
        device = lax.rem(place + k, 16) * stride + lax.rem(me, stride)
        unit_copies.append(copies.start(unit_pos.at[place], unit_pos.at[place], device))

    heavies = []
    for g in range(stride):
        at = jnp.int32(0)
        for k in range(16):
            at = at + jnp.where(counts[g + stride * k] > base, g + stride * k, 0)
        heavies.append(at)
    source = jnp.int32(0)
    for g in range(stride):
        source = source + jnp.where(lax.rem(me, stride) == g, heavies[g], 0)
    heavy_place = jnp.int32(0)
    for k in range(16):
        heavy_place = heavy_place + jnp.where(source >= stride * (k + 1), 1, 0)

    def offset_of(device):
        before = jnp.int32(0)
        for at in heavies:
            before = before + jnp.where(at < device, 1, 0)
        return base * (device + before)

    def tail_row(device):
        piece = lax.div(device, stride) - jnp.where(source < device, 1, 0)
        return jnp.where(source == device, base, spare + unit * piece)

    def tower(features):
        total = None
        for low in range(0, hidden_width, tile):
            act = dot(features, w_first[:, low : low + tile], 1, 0)
            hidden = gelu_and_slope(act)[0].astype(BF16)
            part = dot(hidden, w_second[low : low + tile, :], 1, 0)
            total = part if total is None else total + part
        return total.astype(BF16)

    feat_base[core, 0] = query_features[:base]
    feat_base[core, 1] = passage_features[:base]
    pair_x = [copies.start(feat_base.at[core], feat_base.at[core], partner)]
    wait_all(loads)
    embedded = tower(feat_base[core].reshape(2 * base, width))
    q_base[spot] = embedded[:base]
    p_base[row] = embedded[base:]
    q_copies = [copies.start(q_base.at[spot], q_base.at[spot], device) for device in plane_peers]
    wait_all(mid_copies)
    source_row, source_aside = jnp.int32(0), heavy_place
    for k in range(1, rows):
        beyond = heavy_place >= k * near
        source_row = source_row + jnp.where(beyond, 1, 0)
        source_aside = source_aside - jnp.where(beyond, near, 0)
    unit_pass[...] = jnp.where(source_aside == aside, units[:, aside], unit_mid[source_aside])
    for k in range(1, rows):
        there = lax.rem(row + k, rows)
        unit_copies.append(
            copies.start(unit_pass.at[there], unit_land.at[row], there * plane + spot)
        )
    p_copies = [copies.start(p_base.at[row], p_base.at[row], device) for device in line_peers]

    wait_all(unit_copies)
    heavy = source == me
    got = jnp.where(source_row == row, unit_pass[row], unit_land[source_row]).astype(F32)
    tail_q = jnp.where(heavy, query_features[base:spare].astype(F32), got[:, :width])
    tail_p = jnp.where(heavy, passage_features[base:spare].astype(F32), got[:, width:])
    slots = lax.broadcasted_iota(jnp.int32, (unit, positives.shape[1]), 1)
    chosen = lax.broadcasted_iota(jnp.int32, slots.shape, 0) + tail_row(me)
    tail_pos = jnp.sum(
        jnp.where(slots == chosen, unit_pos[heavy_place], 0.0), axis=1, keepdims=True
    )
    tail_x = jnp.concatenate([tail_q, tail_p], axis=0)
    feat_tail[core] = tail_x.reshape(2, unit, width).astype(BF16)
    tail_e = tower(tail_x.astype(BF16)).astype(F32)
    q_tail[spot] = tail_e[:unit].astype(BF16)
    p_tail[row] = tail_e[unit:].astype(BF16)
    pos_land[spot, 0] = positives[:, :base].astype(F32)
    sub = lax.broadcasted_iota(jnp.int32, (unit, base), 0) + spot * unit
    along = lax.broadcasted_iota(jnp.int32, (unit, base), 1)
    pos_land[spot, 1] = jnp.sum(jnp.where(sub == along, tail_pos, 0.0), axis=0, keepdims=True)
    for device in plane_peers:
        q_copies.append(copies.start(pos_land.at[spot], pos_land.at[spot], device))
        q_copies.append(copies.start(q_tail.at[spot], q_tail.at[spot], device))
    for device in line_peers:
        p_copies.append(copies.start(p_tail.at[row], p_tail.at[row], device))
    pair_x.append(copies.start(feat_tail.at[core], feat_tail.at[core], partner))
    wait_all(q_copies)
    wait_all(p_copies)

    q_rows, p_rows = plane * base, rows * base
    all_q[:q_rows] = q_base[...].reshape(q_rows, embed)
    all_q[q_rows:] = flat_rows(q_tail[...])
    all_p[:p_rows] = p_base[...].reshape(p_rows, embed)
    all_p[p_rows:] = flat_rows(p_tail[...])
    pos_tail = pos_land[0, 1]
    for k in range(1, plane):
        pos_tail = pos_tail + pos_land[k, 1]
    wanted = jnp.concatenate(
        [pos_land[k, 0] for k in range(plane)] + [pos_tail[:, : plane * unit]], axis=1
    )
    line = [plane * k + spot for k in range(rows)]
    ids = jnp.concatenate(
        [lax.broadcasted_iota(jnp.int32, (base, 1), 0) + offset_of(device) for device in line]
        + [
            lax.broadcasted_iota(jnp.int32, (unit, 1), 0) + offset_of(source) + tail_row(device)
            for device in line
        ],
        axis=0,
    ).astype(F32)
    scores[...] = score_scale * dot(all_p[...], all_q[...], 1, 1)
    value = scores[...]
    hit = ids == wanted
    top = jnp.max(value, axis=0, keepdims=True)
    stat_land[spot, 0:1] = top
    stat_land[spot, 1:2] = jnp.sum(jnp.exp(value - top), axis=0, keepdims=True)
    stat_land[spot, 2:3] = jnp.sum(jnp.where(hit, value, 0.0), axis=0, keepdims=True)
    stat_land[spot, 3:4] = jnp.zeros_like(top)
    wait_all(
        [copies.start(stat_land.at[spot], stat_land.at[spot], device) for device in plane_peers]
    )
    stats = stat_land[...]
    tops = stats[:, 0]
    row_top = jnp.max(tops, axis=0, keepdims=True)
    mass = jnp.sum(stats[:, 1] * jnp.exp(tops - row_top), axis=0, keepdims=True)
    log_norm = row_top + jnp.log(mass)
    found = jnp.sum(stats[:, 2], axis=0, keepdims=True)
    loss_land[row] = jnp.broadcast_to(
        jnp.sum(log_norm - found, axis=1, keepdims=True), loss_land.shape[1:]
    )
    grads_t = (jnp.exp(scores[...] - log_norm) - hit.astype(F32)).astype(BF16)

    def scatter(part, own_base, own_tail, out_base, out_tail, land_base, land_tail, mine, peers):
        split = own_base.shape[0] * base
        own_base[...] = part[:split].reshape(own_base.shape)
        own_tail[...] = part[split:].reshape(own_tail.shape)
        out_base[...] = own_base[...].astype(out_base.dtype)
        out_tail[...] = own_tail[...].astype(out_tail.dtype)
        made = []
        for there, device in peers:
            made.append(copies.start(out_base.at[there], land_base.at[mine], device))
            made.append(copies.start(out_tail.at[there], land_tail.at[mine], device))
        return made

    def gathered(own_part, land, mine, members):
        total = own_part[mine]
        for k in range(1, members):
            total = total + land[lax.rem(mine + k, members)].astype(F32)
        return total.astype(BF16)

    dq_copies = scatter(
        score_scale * dot(grads_t, all_p[...], 0, 0),
        dq_own_base,
        dq_own_tail,
        dq_out_base,
        dq_out_tail,
        dq_land_base,
        dq_land_tail,
        spot,
        [(lax.rem(spot + k, plane), plane_peers[k - 1]) for k in range(1, plane)],
    )
    dp_copies = scatter(
        score_scale * dot(grads_t, all_q[...], 1, 0),
        dp_own_base,
        dp_own_tail,
        dp_out_base,
        dp_out_tail,
        dp_land_base,
        dp_land_tail,
        row,
        [(lax.rem(row + k, rows), line_peers[k - 1]) for k in range(1, rows)],
    )
    loss_copies = [
        copies.start(loss_land.at[row], loss_land.at[row], device) for device in line_peers
    ]
    wait_all(pair_x)
    x_rows = 4 * base
    all_x[:x_rows] = feat_base[...].reshape(x_rows, width)
    all_x[x_rows:] = flat_rows(feat_tail[...])
    for t in range(TILES):
        start = pl.multiple_of(core * hidden_half + t * tile, 128)
        hidden, slope = gelu_and_slope(dot(all_x[...], w_first[:, pl.ds(start, tile)], 1, 0))
        all_hidden[t] = hidden.astype(BF16)
        all_slope[t] = slope
    wait_all(dq_copies)
    de_base[core, 0] = gathered(dq_own_base, dq_land_base, spot, plane)
    de_tail[core, 0] = gathered(dq_own_tail, dq_land_tail, spot, plane)

    def send_de(side):
        return [
            copies.start(de_base.at[core, side], de_base.at[core, side], partner),
            copies.start(de_tail.at[core, side], de_tail.at[core, side], partner),
        ]

    pair_de = send_de(0)
    wait_all(dp_copies)
    de_base[core, 1] = gathered(dp_own_base, dp_land_base, row, rows)
    de_tail[core, 1] = gathered(dp_own_tail, dp_land_tail, row, rows)
    pair_de += send_de(1)
    wait_all(loss_copies)
    loss = loss_land[0]
    for k in range(1, rows):
        loss = loss + loss_land[k]
    out_loss[...] = loss * (1.0 / (size * spare))

    def keep(t, part, low):
        high = low + part.shape[1]
        for i in range(per_tile):
            for m in range(lanes):
                for j in range(2):
                    at = ((i * lanes + m) * 2 + j) * chunk
                    piece = part[at : at + chunk]
                    own[t * per_tile + i, m, j, :, low:high] = piece
                    outgoing[t * per_tile + i, m, j, :, low:high] = piece.astype(BF16)
        made = []
        block = pl.ds(t * per_tile, per_tile)
        for k in range(1, lanes):
            there = lax.rem(lane + k, lanes)
            made.append(
                copies.start(
                    outgoing.at[block, there, :, :, pl.ds(low, high - low)],
                    landing.at[lane, block, :, :, pl.ds(low, high - low)],
                    plane * row + 2 * there + core,
                )
            )
        return made

    wait_all(pair_de)
    de = jnp.concatenate([de_base[...].reshape(x_rows, embed), flat_rows(de_tail[...])], axis=0)
    lane_copies = [keep(0, dot(all_hidden[0], de, 0, 0), width)]
    for t in range(TILES):
        start = pl.multiple_of(core * hidden_half + t * tile, 128)
        back = dot(de, w_second[pl.ds(start, tile), :], 1, 1)
        act_grad = (all_slope[t] * back).astype(BF16)
        lane_copies[t] += keep(t, dot(act_grad, all_x[...], 0, 0), 0)
        if t + 1 < TILES:
            lane_copies.append(keep(t + 1, dot(all_hidden[t + 1], de, 0, 0), width))

    sender_core = lax.div(row, half)

    def line_copy(i, j):
        return pltpu.make_async_remote_copy(
            src_ref=forward.at[i, j],
            dst_ref=landed.at[row],
            send_sem=line_send.at[i, j],
            recv_sem=line_recv.at[row],
            device_id=(plane * (half * core + i) + column + j,),
            device_id_type=MESH,
        )

    for t in range(TILES):
        wait_all(lane_copies[t])
        for i in range(t * per_tile, (t + 1) * per_tile):
            for j in range(2):
                total = own[i, lane, j]
                for k in range(1, lanes):
                    total = total + landing[lax.rem(lane + k, lanes), i, j].astype(F32)
                sums[i, j] = total
                forward[i, j] = total.astype(BF16)

                @pl.when(plane * (half * core + i) + column + j != me)
                def _():
                    line_copy(i, j).start()

    for i in range(half):
        for j in range(2):

            @pl.when(plane * (half * core + i) + column + j != me)
            def _():
                line_copy(i, j).wait_send()

    for sender_row in range(rows):
        sender = plane * sender_row + column + sender_core

        @pl.when(sender != me)
        def _():
            pltpu.make_async_remote_copy(
                src_ref=forward.at[0, 0],
                dst_ref=landed.at[sender_row],
                send_sem=line_send.at[0, 0],
                recv_sem=line_recv.at[sender_row],
                device_id=(sender,),
                device_id_type=MESH,
            ).wait_recv()

    total = jnp.where(sender_core == core, sums[lax.rem(row, half), core], 0.0)
    for sender_row in range(rows):
        sender = plane * sender_row + column + sender_core
        total = total + jnp.where(sender == me, 0.0, landed[sender_row].astype(F32))
    out_all[...] = total


def split_kernel(loss, total, mean_loss, first, second):
    width = first.shape[1]
    mean_loss[0] = loss[0, 0]
    first[...] = total[:, :width]
    second[...] = total[:, width:]


def split_outputs(loss, total, width):
    vmem = pl.BlockSpec(memory_space=pltpu.VMEM)
    chunk, across = total.shape
    return pl.pallas_call(
        split_kernel,
        out_shape=[
            jax.ShapeDtypeStruct((1,), F32),
            jax.ShapeDtypeStruct((chunk, width), F32),
            jax.ShapeDtypeStruct((chunk, across - width), F32),
        ],
        in_specs=[pl.BlockSpec(memory_space=pltpu.SMEM), vmem],
        out_specs=[pl.BlockSpec(memory_space=pltpu.SMEM), vmem, vmem],
    )(loss, total)


def step(size, plane, score_scale, counts, *arrays):
    query_features, _, positives, w_first, w_second = arrays
    rows, lanes = size // plane, plane // 2
    half = rows // 2
    width, hidden_width = w_first.shape
    embed = w_second.shape[1]
    chunk = hidden_width // size
    across = width + embed
    base = query_features.shape[0] // 2
    unit = base // 16
    block = base + unit
    vmem = pl.BlockSpec(memory_space=pltpu.VMEM)
    count = 30 + 4 * (plane - 1) + 2 * (rows - 1) + 2
    count += 2 * (plane - 1) + 3 * (rows - 1) + 4 + 2 * TILES * (lanes - 1)

    def split(members, dtype):
        return [
            pltpu.VMEM((members, base, embed), dtype),
            pltpu.VMEM((members, unit, embed), dtype),
        ]

    scratch = [
        pltpu.VMEM((rows, 16 // rows, unit, 2 * width), BF16),
        pltpu.VMEM((16 // rows, rows, unit, 2 * width), BF16),
        pltpu.VMEM((rows, unit, 2 * width), BF16),
        pltpu.VMEM((rows, unit, 2 * width), BF16),
        pltpu.VMEM((16,) + positives.shape, F32),
        pltpu.VMEM((2, 2, base, width), BF16),
        pltpu.VMEM((2, 2, unit, width), BF16),
        *split(plane, BF16),
        *split(rows, BF16),
        pltpu.VMEM((plane, 2, 1, base), F32),
        pltpu.VMEM((plane * block, embed), BF16),
        pltpu.VMEM((rows * block, embed), BF16),
        pltpu.VMEM((rows * block, plane * block), F32),
        pltpu.VMEM((plane, 4, plane * block), F32),
        *split(plane, F32),
        *split(plane, BF16),
        *split(plane, BF16),
        *split(rows, F32),
        *split(rows, BF16),
        *split(rows, BF16),
        pltpu.VMEM((rows, 8, 128), F32),
        pltpu.VMEM((2, 2, base, embed), BF16),
        pltpu.VMEM((2, 2, unit, embed), BF16),
        pltpu.VMEM((4 * block, width), BF16),
        pltpu.VMEM((half, lanes, 2, chunk, across), F32),
        pltpu.VMEM((half, lanes, 2, chunk, across), BF16),
        pltpu.VMEM((lanes, half, 2, chunk, across), BF16),
        pltpu.VMEM((half, 2, chunk, across), F32),
        pltpu.VMEM((half, 2, chunk, across), BF16),
        pltpu.VMEM((rows, chunk, across), BF16),
        pltpu.SemaphoreType.DMA((count,)),
        pltpu.SemaphoreType.DMA((count,)),
        pltpu.SemaphoreType.DMA((half, 2)),
        pltpu.SemaphoreType.DMA((rows,)),
        pltpu.VMEM(w_first.shape, BF16),
        pltpu.VMEM(w_second.shape, BF16),
        pltpu.VMEM((TILES, 4 * block, hidden_width // 2 // TILES), BF16),
        pltpu.VMEM((TILES, 4 * block, hidden_width // 2 // TILES), F32),
        pltpu.SemaphoreType.DMA((2,)),
    ]
    return pl.pallas_call(
        functools.partial(step_kernel, size, plane, score_scale),
        out_shape=[
            jax.ShapeDtypeStruct((8, 128), F32),
            jax.ShapeDtypeStruct((chunk, across), F32),
        ],
        in_specs=[pl.BlockSpec(memory_space=pltpu.SMEM)] + [vmem] * 3
        + [pl.BlockSpec(memory_space=pl.ANY)] * 2,
        out_specs=[vmem] * 2,
        scratch_shapes=scratch,
        compiler_params=pltpu.CompilerParams(
            collective_id=0, has_side_effects=True, vmem_limit_bytes=60 * 1024 * 1024
        ),
    )(counts, *arrays)


def body(query_features, passage_features, counts, positives, w_first, w_second):
    device_count = lax.axis_size("dp")
    plane = 1 << device_count.bit_length() // 2
    score_scale = 2.5 * w_second.shape[1] ** (-0.5)
    loss, total = step(
        device_count,
        plane,
        score_scale,
        counts,
        query_features,
        passage_features,
        positives[None, :],
        w_first,
        w_second,
    )
    mean_loss, grad_first, grad_second = split_outputs(loss, total, w_first.shape[0])
    return (mean_loss[0], grad_first.T, grad_second)


def solution(mesh):
    return jax.shard_map(
        body,
        mesh=mesh,
        in_specs=(P("dp", None), P("dp", None), P(), P("dp"), P(), P()),
        out_specs=(P(), P(None, "dp"), P("dp", None)),
        check_vma=False,
    )
```
